32 devices in a mesh: rep: 2 (over x), dp: 16 (over y, z, core).
Axes of the slice: x: 2, y: 2, z: 4, core: 2. Of those that a mesh axis runs over, the one named last changes fastest.
Arguments:
- x: bfloat16 [32, 2048, 768], P(('rep', 'dp')), parts along dimension 0
- dy: bfloat16 [32, 2048, 768], P(('rep', 'dp')), parts along dimension 0
- w_gate: bfloat16 [2, 768, 1792], replicated
- w_up: bfloat16 [2, 768, 1792], replicated
- w_down: bfloat16 [2, 1792, 768], replicated
- m_w_gate: float32 [2, 768, 1792], P(None, 'dp')
- m_w_up: float32 [2, 768, 1792], P(None, 'dp')
- m_w_down: float32 [2, 1792, 768], P(None, 'dp')
- v_w_gate: float32 [2, 768, 1792], P(None, 'dp')
- v_w_up: float32 [2, 768, 1792], P(None, 'dp')
- v_w_down: float32 [2, 1792, 768], P(None, 'dp')
Outputs:
- output 1: bfloat16 [4, 768, 1792], P('rep'), parts along dimension 0
- output 2: bfloat16 [4, 768, 1792], P('rep'), parts along dimension 0
- output 3: bfloat16 [4, 1792, 768], P('rep'), parts along dimension 0
- output 4: float32 [4, 768, 1792], P('rep', 'dp'), parts along dimension 0
- output 5: float32 [4, 768, 1792], P('rep', 'dp'), parts along dimension 0
- output 6: float32 [4, 1792, 768], P('rep', 'dp'), parts along dimension 0
- output 7: float32 [4, 768, 1792], P('rep', 'dp'), parts along dimension 0
- output 8: float32 [4, 768, 1792], P('rep', 'dp'), parts along dimension 0
- output 9: float32 [4, 1792, 768], P('rep', 'dp'), parts along dimension 0
There are 2 independent parts. The reference program is written for one: setup_inputs(seed, part) draws one part's arguments, and reference() takes and returns one part's arrays. A program takes and returns all parts, laid end to end along the dimension named above; an argument that names none is the same for every part.
All inputs are finite; a program needn't handle non-finite values.
Results may differ from the reference program's by a relative error of at most 0.022.
Values are sent between devices in bfloat16 or wider.
A program may use at most 2 GiB of HBM per device.

```python
import jax
import jax.numpy as jnp
from jax import lax

SEQUENCES = 16
TOKENS = 2048
D = 768
FF = 1792
LAYERS = 2
NAMES = ("w_gate", "w_up", "w_down")
SHAPES = {"w_gate": (LAYERS, D, FF), "w_up": (LAYERS, D, FF), "w_down": (LAYERS, FF, D)}


def bump(key, n, height):
    away = (jnp.arange(n, dtype=jnp.int32) - jax.random.randint(key, (), 0, n, jnp.int32)) % n
    return jnp.where(away < n // 8, height, 1.0)


def together(key, own, strength):
    shared = jax.random.normal(key, own.shape[1:], jnp.float32)
    return (own + strength * shared) * lax.rsqrt(1 + strength * strength)


def setup_inputs(seed: int = 0, part: int = 0) -> dict:
    kx, kdy, ka, kb, kz, kf, kh, kl, *keys = jax.random.split(jax.random.key(seed), 8 + 3 * len(NAMES))
    kx, kdy, ka, kb = (jax.random.fold_in(k, part) for k in (kx, kdy, ka, kb))
    kw, km, kv = (keys[i::3] for i in range(3))
    shape = (SEQUENCES, TOKENS, D)
    much_x, much_dy = jax.random.uniform(kz, (2,), jnp.float32, 0.0, 1.0)
    loud = 2.0 ** jax.random.uniform(jax.random.fold_in(kz, 1), (), jnp.float32, -1.0, 2.0)
    layers = 2.0 ** jax.random.uniform(kl, (LAYERS, 1, 1), jnp.float32, -1.0, 1.0)
    x = together(ka, jax.random.normal(kx, shape, jnp.float32), much_x) * bump(kf, D, 4.0)
    dy = together(kb, jax.random.normal(kdy, shape, jnp.float32), much_dy)
    drawn = {"x": x.astype(jnp.bfloat16), "dy": (loud * dy * (SEQUENCES * TOKENS) ** -0.5).astype(jnp.bfloat16)}
    for key, name in zip(kw, NAMES, strict=True):
        w = jax.random.normal(key, SHAPES[name], jnp.float32) * SHAPES[name][1] ** -0.5
        drawn[name] = (w * {"w_gate": 1.0, "w_up": bump(kh, FF, 4.0), "w_down": layers}[name]).astype(jnp.bfloat16)
    for key, name in zip(km, NAMES, strict=True):
        drawn[f"m_{name}"] = 0.1 * jax.random.normal(key, SHAPES[name], jnp.float32)
    for key, name in zip(kv, NAMES, strict=True):
        drawn[f"v_{name}"] = jax.random.uniform(key, SHAPES[name], jnp.float32, 0.005, 0.015)
    return drawn


def matmul(a, w):
    return jnp.dot(a, w, preferred_element_type=jnp.float32).astype(jnp.bfloat16)


def normed(h):
    wide = h.astype(jnp.float32)
    scale = lax.rsqrt(jnp.mean(wide**2, -1, keepdims=True) + 1e-6)
    return (wide * scale).astype(jnp.bfloat16)


def layer(h, w):
    a = normed(h)
    gate = jnp.dot(a, w["w_gate"], preferred_element_type=jnp.float32)
    up = jnp.dot(a, w["w_up"], preferred_element_type=jnp.float32)
    return h + matmul((jax.nn.silu(gate) * up).astype(jnp.bfloat16), w["w_down"])


def adamw(w, m, v, g):
    m = 0.9 * m + 0.1 * g
    v = 0.95 * v + 0.05 * g * g
    step = m * lax.rsqrt(v + 1e-8) + 0.1 * w
    return (w - 0.02 * step).astype(jnp.bfloat16), m, v


def clipped(gradients, sum_of_squares, count):
    factor = jnp.minimum(1.0, 0.5 * lax.rsqrt(sum_of_squares / count + 1e-30))
    return [g * factor for g in gradients]


def stack(weights, h):
    return lax.scan(lambda h, w: (layer(h, w), None), h, weights)[0]


def reference(x, dy, w_gate, w_up, w_down, m_w_gate, m_w_up, m_w_down, v_w_gate, v_w_up, v_w_down):
    weights = dict(zip(NAMES, (w_gate, w_up, w_down), strict=True))

    def take(so_far, sequence):
        h, by_y = sequence
        _, back = jax.vjp(lambda w: stack(w, h), weights)
        return jax.tree.map(lambda total, term: total + term.astype(jnp.float32), so_far, back(by_y)[0]), None

    none_yet = {name: jnp.zeros(w.shape, jnp.float32) for name, w in weights.items()}
    by_weights, _ = lax.scan(take, none_yet, (x, dy))
    gradients = [by_weights[name].astype(jnp.bfloat16).astype(jnp.float32) for name in NAMES]
    gradients = clipped(gradients, sum(jnp.sum(g * g) for g in gradients), sum(g.size for g in gradients))
    new = [
        adamw(w.astype(jnp.float32), m, v, g)
        for w, m, v, g in zip((w_gate, w_up, w_down), (m_w_gate, m_w_up, m_w_down), (v_w_gate, v_w_up, v_w_down), gradients, strict=True)
    ]
    return tuple(one[which] for which in range(3) for one in new)
```

```python
import functools

import jax
import jax.numpy as jnp
from jax import lax
from jax.experimental import pallas as pl
from jax.experimental.pallas import tpu as pltpu
from jax.sharding import PartitionSpec as P

MESH = pl.DeviceIdType.MESH
Y, Z, C = 2, 4, 2
N = Y * Z * C
F32, BF16 = jnp.float32, jnp.bfloat16


def place():
    me = lax.axis_index("dp")
    return me, me // (Z * C), lax.rem(me // C, Z), lax.rem(me, C)


def index(y, z, c):
    return (y * Z + z) * C + c


def remote(src, dst, send, recv, to):
    return pltpu.make_async_remote_copy(
        src_ref=src, dst_ref=dst, send_sem=send, recv_sem=recv, device_id={"dp": to}, device_id_type=MESH
    )


def update_kernel(count, layers, *refs):
    g, m, v, wf = refs[0:3], refs[3:6], refs[6:9], refs[9:12]
    w_out, m_out, v_out = refs[12:15], refs[15:18], refs[18:21]
    full, own, norms = refs[21:24], refs[24:27], refs[27]
    in_sem, norm_send, norm_recv, send_z, recv_z, send_y, recv_y, send_c, recv_c, out_sem = refs[28:]
    me, y, z, c = place()
    rows = [ref.shape[1] for ref in g]
    loads = []
    for i in range(3):
        loads.append(pltpu.make_async_copy(wf[i].at[:, pl.ds(me * rows[i], rows[i])], own[i], in_sem.at[i]))
        loads[-1].start()

    barrier = pltpu.get_barrier_semaphore()

    def hello(d, _):
        pl.semaphore_signal(barrier, inc=1, device_id={"dp": lax.rem(me + d, N)}, device_id_type=MESH)
        return 0

    lax.fori_loop(1, N, hello, 0)

    total = jnp.zeros((), F32)
    for i in range(3):
        columns = g[i].shape[2]

        def squares(t, acc):
            for l in range(layers):
                part = g[i][l, pl.ds(pl.multiple_of(t * 16, 16), 16), :].astype(F32)
                acc = acc + part * part
            return acc

        acc = lax.fori_loop(0, rows[i] // 16, squares, jnp.zeros((16, columns), F32))
        total = total + jnp.sum(acc)
    norms[pl.ds(me, 1)] = jnp.full((1, 8, 128), total, F32)
    pl.semaphore_wait(barrier, N - 1)

    def tell(d):
        to = lax.rem(me + d, N)
        return remote(norms.at[pl.ds(me, 1)], norms.at[pl.ds(me, 1)], norm_send.at[d], norm_recv.at[d], to)

    lax.fori_loop(1, N, lambda d, _: (tell(d).start(), 0)[1], 0)

    def heard(d, _):
        frm = lax.rem(me + N - d, N)
        copy = remote(norms.at[pl.ds(frm, 1)], norms.at[pl.ds(frm, 1)], norm_send.at[d], norm_recv.at[d], frm)
        copy.wait_recv()
        return 0

    lax.fori_loop(1, N, heard, 0)
    sum_of_squares = jnp.sum(norms[...], axis=0)
    factor = jnp.minimum(1.0, 0.5 * lax.rsqrt(sum_of_squares / count + 1e-30))[0:1, 0:1]
    for load in loads:
        load.wait()
    chunks = [(i, l) for l in range(layers) for i in range(3)]
    mixed = {len(chunks) - 1}

    for i, l in chunks:

        def adamw(t, _):
            at = pl.ds(pl.multiple_of(t * 16, 16), 16)
            grad = g[i][l, at, :].astype(F32) * factor
            w = own[i][l, at, :].astype(F32)
            mm = 0.9 * m[i][l, at, :] + 0.1 * grad
            vv = 0.95 * v[i][l, at, :] + 0.05 * grad * grad
            m_out[i][l, at, :] = mm
            v_out[i][l, at, :] = vv
            new = (w - 0.02 * (mm * lax.rsqrt(vv + 1e-8) + 0.1 * w)).astype(BF16)
            full[i][l, pl.ds(pl.multiple_of(me * rows[i] + t * 16, 16), 16), :] = new
            return 0

        lax.fori_loop(0, rows[i] // 16, adamw, 0)

    def block(k, yy, zz, cc):
        i, l = chunks[k]
        return full[i].at[l, pl.ds(index(yy, zz, cc) * rows[i], rows[i])]

    def origin(slot):
        return z - slot if slot < 4 else z + slot - 3

    def has(slot):
        if slot == 0:
            return z >= 0
        return z >= slot if slot < 4 else z + slot - 3 < Z

    def to_y(k, slot):
        ref = block(k, y, origin(slot), c)
        return remote(ref, ref, send_y.at[k, slot], recv_y.at[k, slot], index(1 - y, z, c))

    def from_y(k, slot):
        ref = block(k, 1 - y, origin(slot), c)
        return remote(ref, ref, send_y.at[k, slot], recv_y.at[k, slot], index(1 - y, z, c))

    def to_c(k, side, slot):
        ref = block(k, y if side == 0 else 1 - y, origin(slot), c)
        return remote(ref, ref, send_c.at[k, side, slot], recv_c.at[k, side, slot], index(y, z, 1 - c))

    def from_c(k, side, slot):
        ref = block(k, y if side == 0 else 1 - y, origin(slot), 1 - c)
        return remote(ref, ref, send_c.at[k, side, slot], recv_c.at[k, side, slot], index(y, z, 1 - c))

    lanes = [(k, 0) for k in range(len(chunks))] + [(k, 1) for k in sorted(mixed)]

    def line(n, slot, up):
        k, side = lanes[n]
        ref = block(k, y if side == 0 else 1 - y, origin(slot), c)
        hop = (slot if slot else 0) if up else (slot - 3 if slot else 0)
        return remote(ref, ref, send_z.at[n, 0 if up else 1, hop], recv_z.at[n, 0 if up else 1, hop],
                      index(y, jnp.minimum(z + 1, Z - 1) if up else jnp.maximum(z - 1, 0), c))

    def arrived(n, slot):
        k, side = lanes[n]
        up = slot < 4
        ref = block(k, y if side == 0 else 1 - y, origin(slot), c)
        hop = slot - 1 if up else slot - 4
        return remote(ref, ref, send_z.at[n, 0 if up else 1, hop], recv_z.at[n, 0 if up else 1, hop],
                      index(y, jnp.maximum(z - 1, 0) if up else jnp.minimum(z + 1, Z - 1), c))

    def when(ok, f):
        pl.when(ok)(f)

    waits = []

    def launch(ok, copy):
        when(ok, lambda: copy().start())
        waits.append((ok, copy))

    def spread(n, slot):
        k, side = lanes[n]
        ok = has(slot)
        if slot < 4:
            launch(ok & (z < Z - 1), lambda: line(n, slot, True))
        if slot == 0 or slot >= 4:
            launch(ok & (z > 0), lambda: line(n, slot, False))
        if side == 0 and (k not in mixed or slot == 0):
            launch(ok, lambda: to_y(k, slot))
        launch(ok, lambda: to_c(k, side, slot))

    order = sorted(range(len(chunks)), key=lambda k: k not in mixed)
    for k in order:
        spread(k, 0)
    for k in sorted(mixed):
        from_y(k, 0).wait_recv()
        spread(lanes.index((k, 1)), 0)
    ranked = sorted(range(len(lanes)), key=lambda n: lanes[n][0] not in mixed)
    for hop in range(1, Z):
        for n in ranked:
            for slot in (hop, hop + 3):
                when(has(slot), lambda: arrived(n, slot).wait_recv())
                spread(n, slot)

    def out(k, side):
        i, l = chunks[k]
        half = pl.ds((y if side == 0 else 1 - y) * (Z * C * rows[i]), Z * C * rows[i])
        return pltpu.make_async_copy(full[i].at[l, half], w_out[i].at[l, half], out_sem.at[k, side])

    slots = [0, 1, 4, 2, 5, 3, 6]
    for k in order:
        for slot in slots:
            when(has(slot), lambda: from_c(k, 0, slot).wait_recv())
        out(k, 0).start()
    for slot in slots:
        for k in order:
            if k not in mixed:
                when(has(slot), lambda: from_y(k, slot).wait_recv())
                launch(has(slot), lambda k=k, slot=slot: to_c(k, 1, slot))
    for k in order:
        for slot in slots:
            when(has(slot), lambda: from_c(k, 1, slot).wait_recv())
        out(k, 1).start()
    for ok, copy in waits:
        when(ok, lambda: copy().wait_send())
    lax.fori_loop(1, N, lambda d, _: (tell(d).wait_send(), 0)[1], 0)
    for k in order:
        for side in range(2):
            out(k, side).wait()


def update(g, m, v, w):
    layers = w[0].shape[0]
    count = float(sum(a.size for a in w))
    vmem = pl.BlockSpec(memory_space=pltpu.VMEM)
    hbm = pl.BlockSpec(memory_space=pl.ANY)
    chunks = 3 * layers
    dma = pltpu.SemaphoreType.DMA
    outs = [jax.ShapeDtypeStruct(a.shape, BF16) for a in w] + [jax.ShapeDtypeStruct(a.shape, F32) for a in (*m, *v)]
    return pl.pallas_call(
        functools.partial(update_kernel, count, layers),
        out_shape=outs,
        in_specs=[vmem] * 9 + [hbm] * 3,
        out_specs=[hbm] * 3 + [vmem] * 6,
        scratch_shapes=[pltpu.VMEM(a.shape, BF16) for a in w]
        + [pltpu.VMEM(a.shape, BF16) for a in g]
        + [pltpu.VMEM((N, 8, 128), F32)]
        + [dma((3,)), dma((N,)), dma((N,)), dma((chunks + 1, 2, Z)), dma((chunks + 1, 2, Z)), dma((chunks, 7)), dma((chunks, 7)),
           dma((chunks, 2, 7)), dma((chunks, 2, 7)), dma((chunks, 2))],
        compiler_params=pltpu.CompilerParams(collective_id=1, has_side_effects=True, vmem_limit_bytes=60 * 1024 * 1024),
        name="update",
    )(*g, *m, *v, *w)


TILE = 256


def gradient_kernel(layers, *refs):
    acts, aTs, dgs, dus, dhs = (refs[i * layers : (i + 1) * layers] for i in range(5))
    refs = refs[5 * layers :]
    outs, refs = refs[0:3], refs[3:]
    wide, tall, from_c, wide_y, tall_y, wide_z, tall_z, tall_c = refs[:8]
    left, right, aT, dh, wide_sum, tall_sum = refs[8:14]
    tile_sem, keep_sem, send_c, recv_c, send_y, recv_y, send_z, recv_z = refs[14:]
    me, y, z, c = place()
    partner, across = index(y, z, 1 - c), index(1 - y, z, c)
    above, below = index(y, jnp.minimum(z + 1, Z - 1), c), index(y, jnp.maximum(z - 1, 0), c)

    units = []
    for l in reversed(range(layers)):
        units += [(2, l, l), (0, l, 2 * l), (1, l, 2 * l + 1)]
    tiles = {k: (acts[l].shape[0] if i == 2 else dgs[l].shape[1]) // TILE for k, (i, l, s) in enumerate(units)}

    def tile(k, t, slot):
        i, l, _ = units[k]
        at = pl.ds(pl.multiple_of(t * TILE, TILE), TILE)
        if i == 2:
            return pltpu.make_async_copy(acts[l].at[at, :], left.at[slot], tile_sem.at[slot])
        return pltpu.make_async_copy((dgs, dus)[i][l].at[:, at], right.at[slot], tile_sem.at[slot])

    def keep(k):
        i, l, _ = units[k]
        if i == 2:
            return pltpu.make_async_copy(dhs[l], dh, keep_sem.at[0])
        return pltpu.make_async_copy(aTs[l], aT, keep_sem.at[1])

    def unit(k, start, stop):
        i, l, s = units[k]

        def body(t, _):
            slot = lax.rem(t, 2)

            @pl.when(t + 1 < tiles[k])
            def _():
                tile(k, t + 1, 1 - slot).start()

            tile(k, t, slot).wait()
            at = pl.ds(pl.multiple_of(t * TILE, TILE), TILE)
            if i == 2:
                tall[s, at, :] = jnp.dot(left[slot], dh[...], preferred_element_type=F32).astype(BF16)
            else:
                wide[s, :, at] = jnp.dot(aT[...], right[slot], preferred_element_type=F32).astype(BF16)
            return 0

        lax.fori_loop(start, stop, body, 0)

    def parts(k):
        i, l, s = units[k]
        if i == 2:
            return tall.at[s], tall_c.at[s], tall_y.at[s], tall_z.at[s], tall_sum
        return wide.at[s], from_c.at[s], wide_y.at[s], wide_z.at[s], wide_sum

    def block(k, yy, zz, cc):
        ref = parts(k)[0]
        rows = ref.shape[0] // N
        return ref.at[pl.ds(pl.multiple_of(index(yy, zz, cc) * rows, rows), rows), :]

    def by_rows(rows, f):
        def body(t, _):
            f(pl.ds(pl.multiple_of(t * 16, 16), 16))
            return 0

        lax.fori_loop(0, rows // 16, body, 0)

    def swap(k, half, zz):
        row = 1 - y if half == 0 else y
        return remote(block(k, row, zz, 1 - c), parts(k)[1].at[half, zz], send_c.at[k, half, zz], recv_c.at[k, half, zz], partner)

    def cross(k, zz):
        return remote(block(k, 1 - y, zz, c), parts(k)[2].at[zz], send_y.at[k, zz], recv_y.at[k, zz], across)

    def pass_up(k, zz):
        return remote(block(k, y, zz, c), parts(k)[3].at[zz], send_z.at[k, zz], recv_z.at[k, zz], above)

    def pass_down(k, zz):
        slot = jnp.where(z - 1 == zz, Z, zz)
        return remote(block(k, y, zz, c), parts(k)[3].at[slot], send_z.at[k, zz], recv_z.at[k, slot], below)

    order = [0, 3, 1, 2]

    def step1(k):
        for half in range(2):
            for zz in order:
                swap(k, half, zz).start()

    def step2(k):
        got = parts(k)[1]
        for zz in order:
            swap(k, 0, zz).wait_recv()
            mine = block(k, 1 - y, zz, c)

            def add(at):
                mine[at, :] = (mine[at, :].astype(F32) + got[0, zz, at, :].astype(F32)).astype(BF16)

            by_rows(mine.shape[0], add)
            cross(k, zz).start()

    def step4(k):
        _, got, over, came, total = parts(k)
        i, l, _ = units[k]
        for zz in order:
            swap(k, 1, zz).wait_recv()
            cross(k, zz).wait_recv()
            mine = block(k, y, zz, c)
            rows = mine.shape[0]

            def first(at):
                total[at, :] = mine[at, :].astype(F32) + got[1, zz, at, :].astype(F32) + over[zz, at, :].astype(F32)

            by_rows(rows, first)

            @pl.when((z <= zz) & (z > 0))
            def _():
                pass_up(k, zz).wait_recv()

                def add(at):
                    total[at, :] += came[zz, at, :].astype(F32)

                by_rows(rows, add)

            @pl.when((z >= zz) & (z < Z - 1))
            def _():
                slot = jnp.where(z == zz, Z, zz)
                remote(mine, came.at[slot], send_z.at[k, zz], recv_z.at[k, slot], above).wait_recv()

                def add(at):
                    total[at, :] += came[slot, at, :].astype(F32)

                by_rows(rows, add)

            @pl.when(z == zz)
            def _():
                def store(at):
                    outs[i][l, at, :] = total[at, :].astype(BF16)

                by_rows(rows, store)

            @pl.when(z != zz)
            def _():
                def store(at):
                    mine[at, :] = total[at, :].astype(BF16)

                by_rows(rows, store)

            @pl.when(z < zz)
            def _():
                pass_up(k, zz).start()

            @pl.when(z > zz)
            def _():
                pass_down(k, zz).start()

    tile(0, 0, 0).start()
    keep(0).start()
    keep(1).start()
    barrier = pltpu.get_barrier_semaphore()
    near = [(partner, z >= 0), (across, z >= 0), (above, z < Z - 1), (below, z > 0)]
    for to, ok in near:

        @pl.when(ok)
        def _():
            pl.semaphore_signal(barrier, inc=1, device_id={"dp": to}, device_id_type=MESH)

    for k in range(len(units)):
        if k > 0:
            tile(k, 0, 0).start()
        if units[k][0] == 2 or units[k][0] == 0:
            if k > 1:
                keep(k).start()
            keep(k).wait()
        if k == 0:
            unit(k, 0, tiles[k])
            pl.semaphore_wait(barrier, 2 + (z < Z - 1).astype(jnp.int32) + (z > 0).astype(jnp.int32))
        else:
            unit(k, 0, 3)
            step2(k - 1)
            unit(k, 3, tiles[k])
        step1(k)
        if k == 3:
            step4(0)
    last = len(units) - 1
    step4(1)
    step2(last)
    for k in range(2, len(units)):
        step4(k)
    for k in range(len(units)):
        for zz in range(Z):
            swap(k, 0, zz).wait_send()
            swap(k, 1, zz).wait_send()
            cross(k, zz).wait_send()

            @pl.when(z != zz)
            def _():
                pass_up(k, zz).wait_send()


def gradients(acts, aTs, dgs, dus, dhs):
    layers = len(acts)
    ff, tokens = acts[0].shape
    d = aTs[0].shape[0]
    vmem = pl.BlockSpec(memory_space=pltpu.VMEM)
    hbm = pl.BlockSpec(memory_space=pl.ANY)
    dma = pltpu.SemaphoreType.DMA
    w, t = 2 * layers, layers
    units = 3 * layers
    wr, tr = d // N, ff // N
    return pl.pallas_call(
        functools.partial(gradient_kernel, layers),
        out_shape=[jax.ShapeDtypeStruct(s, BF16) for s in ((layers, wr, ff), (layers, wr, ff), (layers, tr, d))],
        in_specs=[hbm] * (5 * layers),
        out_specs=[vmem] * 3,
        scratch_shapes=[
            pltpu.VMEM((w, d, ff), BF16),
            pltpu.VMEM((t, ff, d), BF16),
            pltpu.VMEM((w, 2, Z, wr, ff), BF16),
            pltpu.VMEM((w, Z, wr, ff), BF16),
            pltpu.VMEM((t, Z, tr, d), BF16),
            pltpu.VMEM((w, Z + 1, wr, ff), BF16),
            pltpu.VMEM((t, Z + 1, tr, d), BF16),
            pltpu.VMEM((t, 2, Z, tr, d), BF16),
            pltpu.VMEM((2, TILE, tokens), BF16),
            pltpu.VMEM((2, tokens, TILE), BF16),
            pltpu.VMEM((d, tokens), BF16),
            pltpu.VMEM((tokens, d), BF16),
            pltpu.VMEM((wr, ff), F32),
            pltpu.VMEM((tr, d), F32),
            dma((2,)),
            dma((2,)),
            dma((units, 2, Z)),
            dma((units, 2, Z)),
            dma((units, Z)),
            dma((units, Z)),
            dma((units, Z)),
            dma((units, Z + 1)),
        ],
        compiler_params=pltpu.CompilerParams(collective_id=2, has_side_effects=True, vmem_limit_bytes=63 * 1024 * 1024),
        name="gradients",
    )(*acts, *aTs, *dgs, *dus, *dhs)


def dot(a, b):
    return jnp.dot(a, b, preferred_element_type=F32)


def dot_t(a, b):
    return lax.dot_general(a, b, (((1,), (1,)), ((), ())), preferred_element_type=F32)


def tokens_kernel(layers, x_ref, dy_ref, wg, wu, wd, *outs):
    actT, aT, dg, du, dh = (outs[i * layers : (i + 1) * layers] for i in range(5))
    saved = []
    h = x_ref[...]
    for l in range(layers):
        wide = h.astype(F32)
        scale = lax.rsqrt(jnp.mean(wide * wide, -1, keepdims=True) + 1e-6)
        a = (wide * scale).astype(BF16)
        aT[l][...] = a.T
        gate, up = dot(a, wg[l]), dot(a, wu[l])
        s = jax.nn.sigmoid(gate)
        silu = gate * s
        act = (silu * up).astype(BF16)
        actT[l][...] = act.T
        saved.append((wide, scale, silu, up * (s + silu * (1.0 - s))))
        if l + 1 < layers:
            h = (h.astype(F32) + dot(act, wd[l]).astype(BF16).astype(F32)).astype(BF16)
    d = dy_ref[...]
    for l in reversed(range(layers)):
        wide, scale, silu, slope = saved[l]
        if l + 1 < layers:
            dh[l][...] = d
        by_act = dot_t(d, wd[l]).astype(BF16).astype(F32)
        by_gate, by_up = (by_act * slope).astype(BF16), (by_act * silu).astype(BF16)
        dg[l][...] = by_gate
        du[l][...] = by_up
        if l > 0:
            by_a = dot_t(by_gate, wg[l]).astype(BF16).astype(F32) + dot_t(by_up, wu[l]).astype(BF16).astype(F32)
            by_a = by_a.astype(BF16).astype(F32)
            pull = jnp.mean(by_a * wide, -1, keepdims=True)
            back = (by_a * scale - wide * (scale * scale * scale * pull)).astype(BF16)
            d = (d.astype(F32) + back.astype(F32)).astype(BF16)


def through(x, dy, wg, wu, wd):
    layers, dm, ff = wg.shape
    tokens = x.shape[0]
    t = 256
    tall, flat = pl.BlockSpec((t, dm), lambda i: (i, 0)), pl.BlockSpec((t, ff), lambda i: (i, 0))
    whole = lambda w: pl.BlockSpec(w.shape, lambda i: (0, 0, 0), pipeline_mode=pl.Buffered(1))
    shape = lambda *s: jax.ShapeDtypeStruct(s, BF16)
    outs = pl.pallas_call(
        functools.partial(tokens_kernel, layers),
        grid=(tokens // t,),
        in_specs=[tall, tall, whole(wg), whole(wu), whole(wd)],
        out_specs=[pl.BlockSpec((ff, t), lambda i: (0, i))] * layers
        + [pl.BlockSpec((dm, t), lambda i: (0, i))] * layers
        + [flat] * (2 * layers)
        + [tall] * (layers - 1),
        out_shape=[shape(ff, tokens)] * layers + [shape(dm, tokens)] * layers + [shape(tokens, ff)] * (2 * layers) + [shape(tokens, dm)] * (layers - 1),
        compiler_params=pltpu.CompilerParams(dimension_semantics=("arbitrary",), vmem_limit_bytes=63 * 1024 * 1024),
        name="tokens",
    )(x, dy, wg, wu, wd)
    return [list(outs[i * layers : (i + 1) * layers]) for i in range(4)] + [[*outs[4 * layers :], dy]]


def solution(mesh):
    def step(x, dy, *arrays):
        w, m, v = (arrays[i : i + 3] for i in (0, 3, 6))
        g = gradients(*through(x[0], dy[0], *w))
        return tuple(update(g, m, v, w))

    opt = P(None, "dp", None)
    return jax.shard_map(
        step,
        mesh=mesh,
        in_specs=(P(("rep", "dp")), P(("rep", "dp")), P(), P(), P(), *[opt] * 6),
        out_specs=(*[P("rep")] * 3, *[P("rep", "dp")] * 6),
        check_vma=False,
    )
```

```python
import functools

import jax
import jax.numpy as jnp
from jax import lax
from jax.experimental import pallas as pl
from jax.experimental.pallas import tpu as pltpu
from jax.sharding import PartitionSpec as P

MESH = pl.DeviceIdType.MESH
Y, Z, C = 2, 4, 2
N = Y * Z * C
F32, BF16 = jnp.float32, jnp.bfloat16


def place():
    me = lax.axis_index("dp")
    return me, me // (Z * C), lax.rem(me // C, Z), lax.rem(me, C)


def index(y, z, c):
    return (y * Z + z) * C + c


def remote(src, dst, send, recv, to):
    return pltpu.make_async_remote_copy(
        src_ref=src, dst_ref=dst, send_sem=send, recv_sem=recv, device_id={"dp": to}, device_id_type=MESH
    )


def update_kernel(count, layers, *refs):
    g, m, v, wf = refs[0:3], refs[3:6], refs[6:9], refs[9:12]
    full, m_out, v_out = refs[12:15], refs[15:18], refs[18:21]
    own, norms = refs[21:24], refs[24]
    in_sem, norm_send, norm_recv, send_z, recv_z, send_y, recv_y, send_c, recv_c = refs[25:]
    me, y, z, c = place()
    rows = [ref.shape[1] for ref in g]
    loads = []
    for i in range(3):
        loads.append(pltpu.make_async_copy(wf[i].at[:, pl.ds(me * rows[i], rows[i])], own[i], in_sem.at[i]))
        loads[-1].start()

    barrier = pltpu.get_barrier_semaphore()

    def hello(d, _):
        pl.semaphore_signal(barrier, inc=1, device_id={"dp": lax.rem(me + d, N)}, device_id_type=MESH)
        return 0

    lax.fori_loop(1, N, hello, 0)

    total = jnp.zeros((), F32)
    for i in range(3):
        columns = g[i].shape[2]

        def squares(t, acc):
            for l in range(layers):
                part = g[i][l, pl.ds(pl.multiple_of(t * 16, 16), 16), :].astype(F32)
                acc = acc + part * part
            return acc

        acc = lax.fori_loop(0, rows[i] // 16, squares, jnp.zeros((16, columns), F32))
        total = total + jnp.sum(acc)
    norms[pl.ds(me, 1)] = jnp.full((1, 8, 128), total, F32)
    pl.semaphore_wait(barrier, N - 1)

    def tell(d):
        to = lax.rem(me + d, N)
        return remote(norms.at[pl.ds(me, 1)], norms.at[pl.ds(me, 1)], norm_send.at[d], norm_recv.at[d], to)

    lax.fori_loop(1, N, lambda d, _: (tell(d).start(), 0)[1], 0)

    def heard(d, _):
        frm = lax.rem(me + N - d, N)
        copy = remote(norms.at[pl.ds(frm, 1)], norms.at[pl.ds(frm, 1)], norm_send.at[d], norm_recv.at[d], frm)
        copy.wait_recv()
        return 0

    lax.fori_loop(1, N, heard, 0)
    sum_of_squares = jnp.sum(norms[...], axis=0)
    factor = jnp.minimum(1.0, 0.5 * lax.rsqrt(sum_of_squares / count + 1e-30))[0:1, 0:1]
    for load in loads:
        load.wait()
    chunks = [(i, l) for l in range(layers) for i in range(3)]
    mixed = {len(chunks) - 1}

    for i, l in chunks:

        def adamw(t, _):
            at = pl.ds(pl.multiple_of(t * 16, 16), 16)
            grad = g[i][l, at, :].astype(F32) * factor
            w = own[i][l, at, :].astype(F32)
            mm = 0.9 * m[i][l, at, :] + 0.1 * grad
            vv = 0.95 * v[i][l, at, :] + 0.05 * grad * grad
            m_out[i][l, at, :] = mm
            v_out[i][l, at, :] = vv
            new = (w - 0.02 * (mm * lax.rsqrt(vv + 1e-8) + 0.1 * w)).astype(BF16)
            full[i][l, pl.ds(pl.multiple_of(me * rows[i] + t * 16, 16), 16), :] = new
            return 0

        lax.fori_loop(0, rows[i] // 16, adamw, 0)

    def block(k, yy, zz, cc):
        i, l = chunks[k]
        return full[i].at[l, pl.ds(index(yy, zz, cc) * rows[i], rows[i])]

    def origin(slot):
        return z - slot if slot < 4 else z + slot - 3

    def has(slot):
        if slot == 0:
            return z >= 0
        return z >= slot if slot < 4 else z + slot - 3 < Z

    def to_y(k, slot):
        ref = block(k, y, origin(slot), c)
        return remote(ref, ref, send_y.at[k, slot], recv_y.at[k, slot], index(1 - y, z, c))

    def from_y(k, slot):
        ref = block(k, 1 - y, origin(slot), c)
        return remote(ref, ref, send_y.at[k, slot], recv_y.at[k, slot], index(1 - y, z, c))

    def to_c(k, side, slot):
        ref = block(k, y if side == 0 else 1 - y, origin(slot), c)
        return remote(ref, ref, send_c.at[k, side, slot], recv_c.at[k, side, slot], index(y, z, 1 - c))

    def from_c(k, side, slot):
        ref = block(k, y if side == 0 else 1 - y, origin(slot), 1 - c)
        return remote(ref, ref, send_c.at[k, side, slot], recv_c.at[k, side, slot], index(y, z, 1 - c))

    lanes = [(k, 0) for k in range(len(chunks))] + [(k, 1) for k in sorted(mixed)]

    def line(n, slot, up):
        k, side = lanes[n]
        ref = block(k, y if side == 0 else 1 - y, origin(slot), c)
        hop = (slot if slot else 0) if up else (slot - 3 if slot else 0)
        return remote(ref, ref, send_z.at[n, 0 if up else 1, hop], recv_z.at[n, 0 if up else 1, hop],
                      index(y, jnp.minimum(z + 1, Z - 1) if up else jnp.maximum(z - 1, 0), c))

    def arrived(n, slot):
        k, side = lanes[n]
        up = slot < 4
        ref = block(k, y if side == 0 else 1 - y, origin(slot), c)
        hop = slot - 1 if up else slot - 4
        return remote(ref, ref, send_z.at[n, 0 if up else 1, hop], recv_z.at[n, 0 if up else 1, hop],
                      index(y, jnp.maximum(z - 1, 0) if up else jnp.minimum(z + 1, Z - 1), c))

    def when(ok, f):
        pl.when(ok)(f)

    waits = []

    def launch(ok, copy):
        when(ok, lambda: copy().start())
        waits.append((ok, copy))

    def spread(n, slot):
        k, side = lanes[n]
        ok = has(slot)
        if slot < 4:
            launch(ok & (z < Z - 1), lambda: line(n, slot, True))
        if slot == 0 or slot >= 4:
            launch(ok & (z > 0), lambda: line(n, slot, False))
        if side == 0 and (k not in mixed or slot == 0):
            launch(ok, lambda: to_y(k, slot))
        launch(ok, lambda: to_c(k, side, slot))

    order = sorted(range(len(chunks)), key=lambda k: k not in mixed)
    for k in order:
        spread(k, 0)
    for k in sorted(mixed):
        from_y(k, 0).wait_recv()
        spread(lanes.index((k, 1)), 0)
    ranked = sorted(range(len(lanes)), key=lambda n: lanes[n][0] not in mixed)
    for hop in range(1, Z):
        for n in ranked:
            for slot in (hop, hop + 3):
                when(has(slot), lambda: arrived(n, slot).wait_recv())
                spread(n, slot)

    slots = [0, 1, 4, 2, 5, 3, 6]
    for k in order:
        for slot in slots:
            when(has(slot), lambda: from_c(k, 0, slot).wait_recv())
    for slot in slots:
        for k in order:
            if k not in mixed:
                when(has(slot), lambda: from_y(k, slot).wait_recv())
                launch(has(slot), lambda k=k, slot=slot: to_c(k, 1, slot))
    for k in order:
        for slot in slots:
            when(has(slot), lambda: from_c(k, 1, slot).wait_recv())
    for ok, copy in waits:
        when(ok, lambda: copy().wait_send())
    lax.fori_loop(1, N, lambda d, _: (tell(d).wait_send(), 0)[1], 0)


def update(g, m, v, w):
    layers = w[0].shape[0]
    count = float(sum(a.size for a in w))
    vmem = pl.BlockSpec(memory_space=pltpu.VMEM)
    hbm = pl.BlockSpec(memory_space=pl.ANY)
    chunks = 3 * layers
    dma = pltpu.SemaphoreType.DMA
    outs = [pltpu.VMEM(a.shape, BF16) for a in w] + [jax.ShapeDtypeStruct(a.shape, F32) for a in (*m, *v)]
    return pl.pallas_call(
        functools.partial(update_kernel, count, layers),
        out_shape=outs,
        in_specs=[vmem] * 9 + [hbm] * 3,
        out_specs=[vmem] * 9,
        scratch_shapes=[pltpu.VMEM(a.shape, BF16) for a in g]
        + [pltpu.VMEM((N, 8, 128), F32)]
        + [dma((3,)), dma((N,)), dma((N,)), dma((chunks + 1, 2, Z)), dma((chunks + 1, 2, Z)), dma((chunks, 7)), dma((chunks, 7)),
           dma((chunks, 2, 7)), dma((chunks, 2, 7))],
        compiler_params=pltpu.CompilerParams(collective_id=1, has_side_effects=True, vmem_limit_bytes=36 * 1024 * 1024),
        name="update",
    )(*g, *m, *v, *w)


TILE = 256


def gradient_kernel(layers, *refs):
    acts, aTs, dgs, dus, dhs = (refs[i * layers : (i + 1) * layers] for i in range(5))
    refs = refs[5 * layers :]
    outs, refs = refs[0:3], refs[3:]
    wide, tall, from_c, wide_y, tall_y, wide_z, tall_z, tall_c = refs[:8]
    left, right, aT, dh, wide_sum, tall_sum = refs[8:14]
    tile_sem, keep_sem, send_c, recv_c, send_y, recv_y, send_z, recv_z = refs[14:]
    me, y, z, c = place()
    partner, across = index(y, z, 1 - c), index(1 - y, z, c)
    above, below = index(y, jnp.minimum(z + 1, Z - 1), c), index(y, jnp.maximum(z - 1, 0), c)

    units = []
    for l in reversed(range(layers)):
        units += [(2, l, l), (0, l, 2 * l), (1, l, 2 * l + 1)]
    tiles = {k: (acts[l].shape[0] if i == 2 else dgs[l].shape[1]) // TILE for k, (i, l, s) in enumerate(units)}

    def tile(k, t, slot):
        i, l, _ = units[k]
        at = pl.ds(pl.multiple_of(t * TILE, TILE), TILE)
        if i == 2:
            return pltpu.make_async_copy(acts[l].at[at, :], left.at[slot], tile_sem.at[slot])
        return pltpu.make_async_copy((dgs, dus)[i][l].at[:, at], right.at[slot], tile_sem.at[slot])

    def keep(k):
        i, l, _ = units[k]
        if i == 2:
            return pltpu.make_async_copy(dhs[l], dh, keep_sem.at[0])
        return pltpu.make_async_copy(aTs[l], aT, keep_sem.at[1])

    def unit(k, start, stop):
        i, l, s = units[k]

        def body(t, _):
            slot = lax.rem(t, 2)

            @pl.when(t + 1 < tiles[k])
            def _():
                tile(k, t + 1, 1 - slot).start()

            tile(k, t, slot).wait()
            at = pl.ds(pl.multiple_of(t * TILE, TILE), TILE)
            if i == 2:
                tall[s, at, :] = jnp.dot(left[slot], dh[...], preferred_element_type=F32).astype(BF16)
            else:
                wide[s, :, at] = jnp.dot(aT[...], right[slot], preferred_element_type=F32).astype(BF16)
            return 0

        lax.fori_loop(start, stop, body, 0)

    def parts(k):
        i, l, s = units[k]
        if i == 2:
            return tall.at[s], tall_c.at[s], tall_y.at[s], tall_z.at[s], tall_sum
        return wide.at[s], from_c.at[s], wide_y.at[s], wide_z.at[s], wide_sum

    def block(k, yy, zz, cc):
        ref = parts(k)[0]
        rows = ref.shape[0] // N
        return ref.at[pl.ds(pl.multiple_of(index(yy, zz, cc) * rows, rows), rows), :]

    def by_rows(rows, f):
        def body(t, _):
            f(pl.ds(pl.multiple_of(t * 16, 16), 16))
            return 0

        lax.fori_loop(0, rows // 16, body, 0)

    end = (z == 0) | (z == Z - 1)

    def piece(n):
        far = (jnp.where(z < 2, Z - 1, 0), jnp.where(end, jnp.where(z == 0, 2, 1), jnp.where(z == 1, 0, Z - 1)), jnp.where(end, Z - 2 - jnp.where(z == 0, 1, 0), 3 - z), z)
        return far[n]

    def swap(k, half, n):
        zz = piece(n)
        row = 1 - y if half == 0 else y
        return remote(block(k, row, zz, 1 - c), parts(k)[1].at[half, zz], send_c.at[k, half, n], recv_c.at[k, half, n], partner)

    def cross(k, n):
        zz = piece(n)
        return remote(block(k, 1 - y, zz, c), parts(k)[2].at[zz], send_y.at[k, n], recv_y.at[k, n], across)

    def pass_on(k, n):
        zz = piece(n)
        slot = jnp.where(z - 1 == zz, Z, zz)
        return remote(block(k, y, zz, c), parts(k)[3].at[slot], send_z.at[k, n], recv_z.at[k, slot], jnp.where(zz > z, above, below))

    def passed(k, slot):
        ref = parts(k)[3].at[slot]
        return remote(ref, ref, send_z.at[k, 0], recv_z.at[k, slot], jnp.where(end, jnp.where(z == 0, above, below), above))

    def step1(k):
        for half in range(2):
            for n in range(Z):
                swap(k, half, n).start()

    def step2(k):
        got = parts(k)[1]
        for n in range(Z):
            zz = piece(n)
            swap(k, 0, n).wait_recv()
            mine = block(k, 1 - y, zz, c)

            def add(at):
                mine[at, :] = (mine[at, :].astype(F32) + got[0, zz, at, :].astype(F32)).astype(BF16)

            by_rows(mine.shape[0], add)
            cross(k, n).start()

    def gather(k, n):
        _, got, over, _, total = parts(k)
        zz = piece(n)
        swap(k, 1, n).wait_recv()
        cross(k, n).wait_recv()
        mine = block(k, y, zz, c)

        def first(at):
            total[at, :] = mine[at, :].astype(F32) + got[1, zz, at, :].astype(F32) + over[zz, at, :].astype(F32)

        by_rows(mine.shape[0], first)
        return mine, total

    def also(k, ok, slot):
        _, _, _, came, total = parts(k)

        @pl.when(ok)
        def _():
            passed(k, slot).wait_recv()

            def add(at):
                total[at, :] += came[slot, at, :].astype(F32)

            by_rows(total.shape[0], add)

    def step3(k):
        for n in range(Z - 1):
            mine, total = gather(k, n)
            also(k, jnp.logical_not(end), piece(n))

            def store(at):
                mine[at, :] = total[at, :].astype(BF16)

            by_rows(mine.shape[0], store)
            pass_on(k, n).start()

    def step4(k):
        i, l, _ = units[k]
        mine, total = gather(k, Z - 1)
        also(k, z > 0, z)
        also(k, z < Z - 1, Z)

        def store(at):
            outs[i][l, at, :] = total[at, :].astype(BF16)

        by_rows(mine.shape[0], store)

    tile(0, 0, 0).start()
    keep(0).start()
    keep(1).start()
    barrier = pltpu.get_barrier_semaphore()
    near = [(partner, z >= 0), (across, z >= 0), (above, z < Z - 1), (below, z > 0)]
    for to, ok in near:

        @pl.when(ok)
        def _():
            pl.semaphore_signal(barrier, inc=1, device_id={"dp": to}, device_id_type=MESH)

    for k in range(len(units)):
        if k > 0:
            tile(k, 0, 0).start()
        if units[k][0] == 2 or units[k][0] == 0:
            if k > 1:
                keep(k).start()
            keep(k).wait()
        if k == 0:
            unit(k, 0, tiles[k])
            pl.semaphore_wait(barrier, 2 + (z < Z - 1).astype(jnp.int32) + (z > 0).astype(jnp.int32))
        else:
            unit(k, 0, 3)
            step2(k - 1)
            unit(k, 3, tiles[k])
        step1(k)
        if k in (3, 4):
            step3(k - 3)
    last = len(units) - 1
    step2(last)
    for k in range(2, len(units)):
        step3(k)
        step4(k - 2)
    step4(last - 1)
    step4(last)
    for k in range(len(units)):
        for n in range(Z):
            swap(k, 0, n).wait_send()
            swap(k, 1, n).wait_send()
            cross(k, n).wait_send()
            if n < Z - 1:
                pass_on(k, n).wait_send()


def gradients(acts, aTs, dgs, dus, dhs):
    layers = len(acts)
    ff, tokens = acts[0].shape
    d = aTs[0].shape[0]
    vmem = pl.BlockSpec(memory_space=pltpu.VMEM)
    hbm = pl.BlockSpec(memory_space=pl.ANY)
    dma = pltpu.SemaphoreType.DMA
    w, t = 2 * layers, layers
    units = 3 * layers
    wr, tr = d // N, ff // N
    return pl.pallas_call(
        functools.partial(gradient_kernel, layers),
        out_shape=[pltpu.VMEM(s, BF16) for s in ((layers, wr, ff), (layers, wr, ff), (layers, tr, d))],
        in_specs=[hbm] * (5 * layers),
        out_specs=[vmem] * 3,
        scratch_shapes=[
            pltpu.VMEM((w, d, ff), BF16),
            pltpu.VMEM((t, ff, d), BF16),
            pltpu.VMEM((w, 2, Z, wr, ff), BF16),
            pltpu.VMEM((w, Z, wr, ff), BF16),
            pltpu.VMEM((t, Z, tr, d), BF16),
            pltpu.VMEM((w, Z + 1, wr, ff), BF16),
            pltpu.VMEM((t, Z + 1, tr, d), BF16),
            pltpu.VMEM((t, 2, Z, tr, d), BF16),
            pltpu.VMEM((2, TILE, tokens), BF16),
            pltpu.VMEM((2, tokens, TILE), BF16),
            pltpu.VMEM((d, tokens), BF16),
            pltpu.VMEM((tokens, d), BF16),
            pltpu.VMEM((wr, ff), F32),
            pltpu.VMEM((tr, d), F32),
            dma((2,)),
            dma((2,)),
            dma((units, 2, Z)),
            dma((units, 2, Z)),
            dma((units, Z)),
            dma((units, Z)),
            dma((units, Z)),
            dma((units, Z + 1)),
        ],
        compiler_params=pltpu.CompilerParams(collective_id=2, has_side_effects=True, vmem_limit_bytes=60 * 1024 * 1024),
        name="gradients",
    )(*acts, *aTs, *dgs, *dus, *dhs)


def dot(a, b):
    return jnp.dot(a, b, preferred_element_type=F32)


def dot_t(a, b):
    return lax.dot_general(a, b, (((1,), (1,)), ((), ())), preferred_element_type=F32)


def tokens_kernel(layers, x_ref, dy_ref, wg, wu, wd, *outs):
    actT, aT, dg, du, dh = (outs[i * layers : (i + 1) * layers] for i in range(5))
    saved = []
    h = x_ref[...]
    for l in range(layers):
        wide = h.astype(F32)
        scale = lax.rsqrt(jnp.mean(wide * wide, -1, keepdims=True) + 1e-6)
        a = (wide * scale).astype(BF16)
        aT[l][...] = a.T
        gate, up = dot(a, wg[l]), dot(a, wu[l])
        s = jax.nn.sigmoid(gate)
        silu = gate * s
        act = (silu * up).astype(BF16)
        actT[l][...] = act.T
        saved.append((wide, scale, silu, up * (s + silu * (1.0 - s))))
        if l + 1 < layers:
            h = (h.astype(F32) + dot(act, wd[l]).astype(BF16).astype(F32)).astype(BF16)
    d = dy_ref[...]
    for l in reversed(range(layers)):
        wide, scale, silu, slope = saved[l]
        if l + 1 < layers:
            dh[l][...] = d
        by_act = dot_t(d, wd[l]).astype(BF16).astype(F32)
        by_gate, by_up = (by_act * slope).astype(BF16), (by_act * silu).astype(BF16)
        dg[l][...] = by_gate
        du[l][...] = by_up
        if l > 0:
            by_a = dot_t(by_gate, wg[l]).astype(BF16).astype(F32) + dot_t(by_up, wu[l]).astype(BF16).astype(F32)
            by_a = by_a.astype(BF16).astype(F32)
            pull = jnp.mean(by_a * wide, -1, keepdims=True)
            back = (by_a * scale - wide * (scale * scale * scale * pull)).astype(BF16)
            d = (d.astype(F32) + back.astype(F32)).astype(BF16)


def through(x, dy, wg, wu, wd):
    layers, dm, ff = wg.shape
    tokens = x.shape[0]
    t = 256
    tall, flat = pl.BlockSpec((t, dm), lambda i: (i, 0)), pl.BlockSpec((t, ff), lambda i: (i, 0))
    whole = lambda w: pl.BlockSpec(w.shape, lambda i: (0, 0, 0), pipeline_mode=pl.Buffered(1))
    shape = lambda *s: jax.ShapeDtypeStruct(s, BF16)
    outs = pl.pallas_call(
        functools.partial(tokens_kernel, layers),
        grid=(tokens // t,),
        in_specs=[tall, tall, whole(wg), whole(wu), whole(wd)],
        out_specs=[pl.BlockSpec((ff, t), lambda i: (0, i))] * layers
        + [pl.BlockSpec((dm, t), lambda i: (0, i))] * layers
        + [flat] * (2 * layers)
        + [tall] * (layers - 1),
        out_shape=[shape(ff, tokens)] * layers + [shape(dm, tokens)] * layers + [shape(tokens, ff)] * (2 * layers) + [shape(tokens, dm)] * (layers - 1),
        compiler_params=pltpu.CompilerParams(dimension_semantics=("arbitrary",), vmem_limit_bytes=63 * 1024 * 1024),
        name="tokens",
    )(x, dy, wg, wu, wd)
    return [list(outs[i * layers : (i + 1) * layers]) for i in range(4)] + [[*outs[4 * layers :], dy]]


def solution(mesh):
    def step(x, dy, *arrays):
        w, m, v = (arrays[i : i + 3] for i in (0, 3, 6))
        g = gradients(*through(x[0], dy[0], *w))
        return tuple(update(g, m, v, w))

    opt = P(None, "dp", None)
    return jax.shard_map(
        step,
        mesh=mesh,
        in_specs=(P(("rep", "dp")), P(("rep", "dp")), P(), P(), P(), *[opt] * 6),
        out_specs=(*[P("rep")] * 3, *[P("rep", "dp")] * 6),
        check_vma=False,
    )
```

```python
import functools

import jax
import jax.numpy as jnp
from jax import lax
from jax.experimental import pallas as pl
from jax.experimental.pallas import tpu as pltpu
from jax.sharding import PartitionSpec as P

MESH = pl.DeviceIdType.MESH
Y, Z, C = 2, 4, 2
N = Y * Z * C
F32, BF16 = jnp.float32, jnp.bfloat16


def place():
    me = lax.axis_index("dp")
    return me, me // (Z * C), lax.rem(me // C, Z), lax.rem(me, C)


def index(y, z, c):
    return (y * Z + z) * C + c


def remote(src, dst, send, recv, to):
    return pltpu.make_async_remote_copy(
        src_ref=src, dst_ref=dst, send_sem=send, recv_sem=recv, device_id={"dp": to}, device_id_type=MESH
    )


def update_kernel(count, layers, *refs):
    g, m, v, wf = refs[0:3], refs[3:6], refs[6:9], refs[9:12]
    full, m_out, v_out = refs[12:15], refs[15:18], refs[18:21]
    own, norms = refs[21:24], refs[24]
    in_sem, norm_send, norm_recv, send_z, recv_z, send_y, recv_y, send_c, recv_c = refs[25:]
    me, y, z, c = place()
    rows = [ref.shape[1] for ref in g]
    loads = []
    for i in range(3):
        loads.append(pltpu.make_async_copy(wf[i].at[:, pl.ds(me * rows[i], rows[i])], own[i], in_sem.at[i]))
        loads[-1].start()

    barrier = pltpu.get_barrier_semaphore()

    def hello(d, _):
        pl.semaphore_signal(barrier, inc=1, device_id={"dp": lax.rem(me + d, N)}, device_id_type=MESH)
        return 0

    lax.fori_loop(1, N, hello, 0)

    total = jnp.zeros((), F32)
    for i in range(3):
        columns = g[i].shape[2]

        def squares(t, acc):
            for l in range(layers):
                part = g[i][l, pl.ds(pl.multiple_of(t * 16, 16), 16), :].astype(F32)
                acc = acc + part * part
            return acc

        acc = lax.fori_loop(0, rows[i] // 16, squares, jnp.zeros((16, columns), F32))
        total = total + jnp.sum(acc)
    norms[pl.ds(me, 1)] = jnp.full((1, 8, 128), total, F32)
    pl.semaphore_wait(barrier, N - 1)

    def tell(d):
        to = lax.rem(me + d, N)
        return remote(norms.at[pl.ds(me, 1)], norms.at[pl.ds(me, 1)], norm_send.at[d], norm_recv.at[d], to)

    lax.fori_loop(1, N, lambda d, _: (tell(d).start(), 0)[1], 0)

    def heard(d, _):
        frm = lax.rem(me + N - d, N)
        copy = remote(norms.at[pl.ds(frm, 1)], norms.at[pl.ds(frm, 1)], norm_send.at[d], norm_recv.at[d], frm)
        copy.wait_recv()
        return 0

    lax.fori_loop(1, N, heard, 0)
    sum_of_squares = jnp.sum(norms[...], axis=0)
    factor = jnp.minimum(1.0, 0.5 * lax.rsqrt(sum_of_squares / count + 1e-30))[0:1, 0:1]
    for load in loads:
        load.wait()
    chunks = [(i, l) for l in range(layers) for i in range(3)]
    mixed = {len(chunks) - 1}

    def block(k, yy, zz, cc):
        i, l = chunks[k]
        return full[i].at[l, pl.ds(index(yy, zz, cc) * rows[i], rows[i])]

    def origin(slot):
        return z - slot if slot < 4 else z + slot - 3

    def has(slot):
        if slot == 0:
            return z >= 0
        return z >= slot if slot < 4 else z + slot - 3 < Z

    def to_y(k, slot):
        ref = block(k, y, origin(slot), c)
        return remote(ref, ref, send_y.at[k, slot], recv_y.at[k, slot], index(1 - y, z, c))

    def from_y(k, slot):
        ref = block(k, 1 - y, origin(slot), c)
        return remote(ref, ref, send_y.at[k, slot], recv_y.at[k, slot], index(1 - y, z, c))

    def to_c(k, side, slot):
        ref = block(k, y if side == 0 else 1 - y, origin(slot), c)
        return remote(ref, ref, send_c.at[k, side, slot], recv_c.at[k, side, slot], index(y, z, 1 - c))

    def from_c(k, side, slot):
        ref = block(k, y if side == 0 else 1 - y, origin(slot), 1 - c)
        return remote(ref, ref, send_c.at[k, side, slot], recv_c.at[k, side, slot], index(y, z, 1 - c))

    lanes = [(k, 0) for k in range(len(chunks))] + [(k, 1) for k in sorted(mixed)]

    def line(n, slot, up):
        k, side = lanes[n]
        ref = block(k, y if side == 0 else 1 - y, origin(slot), c)
        hop = (slot if slot else 0) if up else (slot - 3 if slot else 0)
        return remote(ref, ref, send_z.at[n, 0 if up else 1, hop], recv_z.at[n, 0 if up else 1, hop],
                      index(y, jnp.minimum(z + 1, Z - 1) if up else jnp.maximum(z - 1, 0), c))

    def arrived(n, slot):
        k, side = lanes[n]
        up = slot < 4
        ref = block(k, y if side == 0 else 1 - y, origin(slot), c)
        hop = slot - 1 if up else slot - 4
        return remote(ref, ref, send_z.at[n, 0 if up else 1, hop], recv_z.at[n, 0 if up else 1, hop],
                      index(y, jnp.maximum(z - 1, 0) if up else jnp.minimum(z + 1, Z - 1), c))

    def when(ok, f):
        pl.when(ok)(f)

    waits = []

    def launch(ok, copy):
        when(ok, lambda: copy().start())
        waits.append((ok, copy))

    def spread(n, slot):
        k, side = lanes[n]
        ok = has(slot)
        if slot < 4:
            launch(ok & (z < Z - 1), lambda: line(n, slot, True))
        if slot == 0 or slot >= 4:
            launch(ok & (z > 0), lambda: line(n, slot, False))
        if side == 0 and (k not in mixed or slot == 0):
            launch(ok, lambda: to_y(k, slot))
        launch(ok, lambda: to_c(k, side, slot))

    order = sorted(range(len(chunks)), key=lambda k: k not in mixed)
    def renew(i, l):
        def adamw(t, _):
            at = pl.ds(pl.multiple_of(t * 16, 16), 16)
            grad = g[i][l, at, :].astype(F32) * factor
            w = own[i][l, at, :].astype(F32)
            mm = 0.9 * m[i][l, at, :] + 0.1 * grad
            vv = 0.95 * v[i][l, at, :] + 0.05 * grad * grad
            m_out[i][l, at, :] = mm
            v_out[i][l, at, :] = vv
            new = (w - 0.02 * (mm * lax.rsqrt(vv + 1e-8) + 0.1 * w)).astype(BF16)
            full[i][l, pl.ds(pl.multiple_of(me * rows[i] + t * 16, 16), 16), :] = new
            return 0

        lax.fori_loop(0, rows[i] // 16, adamw, 0)

    for k in order:
        renew(*chunks[k])
        spread(k, 0)
    for k in sorted(mixed):
        from_y(k, 0).wait_recv()
        spread(lanes.index((k, 1)), 0)
    ranked = sorted(range(len(lanes)), key=lambda n: lanes[n][0] in mixed)
    for hop in range(1, Z):
        for n in ranked:
            for slot in (hop, hop + 3):
                when(has(slot), lambda: arrived(n, slot).wait_recv())
                spread(n, slot)

    slots = [0, 1, 4, 2, 5, 3, 6]
    for k in order:
        for slot in slots:
            when(has(slot), lambda: from_c(k, 0, slot).wait_recv())
    for slot in slots:
        for k in order:
            if k not in mixed:
                when(has(slot), lambda: from_y(k, slot).wait_recv())
                launch(has(slot), lambda k=k, slot=slot: to_c(k, 1, slot))
    for k in order:
        for slot in slots:
            when(has(slot), lambda: from_c(k, 1, slot).wait_recv())
    for ok, copy in waits:
        when(ok, lambda: copy().wait_send())
    lax.fori_loop(1, N, lambda d, _: (tell(d).wait_send(), 0)[1], 0)


def update(g, m, v, w):
    layers = w[0].shape[0]
    count = float(sum(a.size for a in w))
    vmem = pl.BlockSpec(memory_space=pltpu.VMEM)
    hbm = pl.BlockSpec(memory_space=pl.ANY)
    chunks = 3 * layers
    dma = pltpu.SemaphoreType.DMA
    outs = [pltpu.VMEM(a.shape, BF16) for a in w] + [jax.ShapeDtypeStruct(a.shape, F32) for a in (*m, *v)]
    return pl.pallas_call(
        functools.partial(update_kernel, count, layers),
        out_shape=outs,
        in_specs=[vmem] * 9 + [hbm] * 3,
        out_specs=[vmem] * 9,
        scratch_shapes=[pltpu.VMEM(a.shape, BF16) for a in g]
        + [pltpu.VMEM((N, 8, 128), F32)]
        + [dma((3,)), dma((N,)), dma((N,)), dma((chunks + 1, 2, Z)), dma((chunks + 1, 2, Z)), dma((chunks, 7)), dma((chunks, 7)),
           dma((chunks, 2, 7)), dma((chunks, 2, 7))],
        compiler_params=pltpu.CompilerParams(collective_id=1, has_side_effects=True, vmem_limit_bytes=36 * 1024 * 1024),
        name="update",
    )(*g, *m, *v, *w)


TILE = 256


def gradient_kernel(layers, *refs):
    acts, aTs, dgs, dus, dhs = (refs[i * layers : (i + 1) * layers] for i in range(5))
    refs = refs[5 * layers :]
    outs, refs = refs[0:3], refs[3:]
    wide, tall, from_c, wide_y, tall_y, wide_z, tall_z, tall_c = refs[:8]
    left, right, aT, dh, wide_sum, tall_sum = refs[8:14]
    tile_sem, keep_sem, send_c, recv_c, send_y, recv_y, send_z, recv_z = refs[14:]
    me, y, z, c = place()
    partner, across = index(y, z, 1 - c), index(1 - y, z, c)
    above, below = index(y, jnp.minimum(z + 1, Z - 1), c), index(y, jnp.maximum(z - 1, 0), c)

    units = []
    for l in reversed(range(layers)):
        units += [(2, l, l), (0, l, 2 * l), (1, l, 2 * l + 1)]
    tiles = [2 * Z if i == 2 else dgs[l].shape[1] // TILE for i, l, _ in units]
    tall_tile = acts[0].shape[0] // (2 * Z)

    def rows_of(t):
        return pl.ds(pl.multiple_of(lax.rem(t + Z * (1 - y), 2 * Z) * tall_tile, tall_tile), tall_tile)

    def tile(k, t, slot):
        i, l, _ = units[k]
        if i == 2:
            return pltpu.make_async_copy(acts[l].at[rows_of(t), :], left.at[slot], tile_sem.at[slot])
        at = pl.ds(pl.multiple_of(t * TILE, TILE), TILE)
        return pltpu.make_async_copy((dgs, dus)[i][l].at[:, at], right.at[slot], tile_sem.at[slot])

    def keep(k):
        i, l, _ = units[k]
        if i == 2:
            return pltpu.make_async_copy(dhs[l], dh, keep_sem.at[0])
        return pltpu.make_async_copy(aTs[l], aT, keep_sem.at[1])

    def unit(k, start, stop):
        i, l, s = units[k]

        def body(t, _):
            slot = lax.rem(t, 2)

            @pl.when(t + 1 < tiles[k])
            def _():
                tile(k, t + 1, 1 - slot).start()

            tile(k, t, slot).wait()
            at = pl.ds(pl.multiple_of(t * TILE, TILE), TILE)
            if i == 2:
                tall[s, rows_of(t), :] = jnp.dot(left[slot], dh[...], preferred_element_type=F32).astype(BF16)
            else:
                wide[s, :, at] = jnp.dot(aT[...], right[slot], preferred_element_type=F32).astype(BF16)
            return 0

        lax.fori_loop(start, stop, body, 0)

    def parts(k):
        i, l, s = units[k]
        if i == 2:
            return tall.at[s], tall_c.at[s], tall_y.at[s], tall_z.at[s], tall_sum
        return wide.at[s], from_c.at[s], wide_y.at[s], wide_z.at[s], wide_sum

    def block(k, yy, zz, cc):
        ref = parts(k)[0]
        rows = ref.shape[0] // N
        return ref.at[pl.ds(pl.multiple_of(index(yy, zz, cc) * rows, rows), rows), :]

    def by_rows(rows, f):
        def body(t, _):
            f(pl.ds(pl.multiple_of(t * 16, 16), 16))
            return 0

        lax.fori_loop(0, rows // 16, body, 0)

    end = (z == 0) | (z == Z - 1)

    def piece(n):
        far = (jnp.where(z < 2, Z - 1, 0), jnp.where(end, jnp.where(z == 0, 2, 1), jnp.where(z == 1, 0, Z - 1)), jnp.where(end, Z - 2 - jnp.where(z == 0, 1, 0), 3 - z), z)
        return far[n]

    def swap(k, half, n):
        zz = piece(n)
        row = 1 - y if half == 0 else y
        return remote(block(k, row, zz, 1 - c), parts(k)[1].at[half, zz], send_c.at[k, half, n], recv_c.at[k, half, n], partner)

    def cross(k, n):
        zz = piece(n)
        return remote(block(k, 1 - y, zz, c), parts(k)[2].at[zz], send_y.at[k, n], recv_y.at[k, n], across)

    def pass_on(k, n):
        zz = piece(n)
        slot = jnp.where(z - 1 == zz, Z, zz)
        return remote(block(k, y, zz, c), parts(k)[3].at[slot], send_z.at[k, n], recv_z.at[k, slot], jnp.where(zz > z, above, below))

    def passed(k, slot):
        ref = parts(k)[3].at[slot]
        return remote(ref, ref, send_z.at[k, 0], recv_z.at[k, slot], jnp.where(end, jnp.where(z == 0, above, below), above))

    def step1(k, half):
        for n in range(Z):
            swap(k, half, n).start()

    def step2(k):
        got = parts(k)[1]
        for n in range(Z):
            zz = piece(n)
            swap(k, 0, n).wait_recv()
            mine = block(k, 1 - y, zz, c)

            def add(at):
                mine[at, :] = (mine[at, :].astype(F32) + got[0, zz, at, :].astype(F32)).astype(BF16)

            by_rows(mine.shape[0], add)
            cross(k, n).start()

    def gather(k, n):
        _, got, over, _, total = parts(k)
        zz = piece(n)
        swap(k, 1, n).wait_recv()
        cross(k, n).wait_recv()
        mine = block(k, y, zz, c)

        def first(at):
            total[at, :] = mine[at, :].astype(F32) + got[1, zz, at, :].astype(F32) + over[zz, at, :].astype(F32)

        by_rows(mine.shape[0], first)
        return mine, total

    def also(k, ok, slot):
        _, _, _, came, total = parts(k)

        @pl.when(ok)
        def _():
            passed(k, slot).wait_recv()

            def add(at):
                total[at, :] += came[slot, at, :].astype(F32)

            by_rows(total.shape[0], add)

    def step3(k):
        for n in range(Z - 1):
            mine, total = gather(k, n)
            also(k, jnp.logical_not(end), piece(n))

            def store(at):
                mine[at, :] = total[at, :].astype(BF16)

            by_rows(mine.shape[0], store)
            pass_on(k, n).start()

    def step4(k):
        i, l, _ = units[k]
        mine, total = gather(k, Z - 1)
        also(k, z > 0, z)
        also(k, z < Z - 1, Z)

        def store(at):
            outs[i][l, at, :] = total[at, :].astype(BF16)

        by_rows(mine.shape[0], store)

    tile(0, 0, 0).start()
    keep(0).start()
    keep(1).start()
    barrier = pltpu.get_barrier_semaphore()
    near = [(partner, z >= 0), (across, z >= 0), (above, z < Z - 1), (below, z > 0)]
    for to, ok in near:

        @pl.when(ok)
        def _():
            pl.semaphore_signal(barrier, inc=1, device_id={"dp": to}, device_id_type=MESH)

    for k in range(len(units)):
        if k > 0:
            tile(k, 0, 0).start()
        if units[k][0] == 2 or units[k][0] == 0:
            if k > 1:
                keep(k).start()
            keep(k).wait()
        if k == 0:
            unit(k, 0, Z)
            pl.semaphore_wait(barrier, 2 + (z < Z - 1).astype(jnp.int32) + (z > 0).astype(jnp.int32))
            step1(k, 0)
            unit(k, Z, Z + 2)
            step2(k)
            unit(k, Z + 2, tiles[k])
            step1(k, 1)
        elif k == 1:
            unit(k, 0, tiles[k])
            step1(k, 0)
            step1(k, 1)
        else:
            unit(k, 0, 3)
            step2(k - 1)
            unit(k, 3, tiles[k])
            step1(k, 0)
            step1(k, 1)
        if k in (3, 4):
            step3(k - 3)
    last = len(units) - 1
    step2(last)
    for k in range(2, len(units)):
        step3(k)
        step4(k - 2)
    step4(last - 1)
    step4(last)
    for k in range(len(units)):
        for n in range(Z):
            swap(k, 0, n).wait_send()
            swap(k, 1, n).wait_send()
            cross(k, n).wait_send()
            if n < Z - 1:
                pass_on(k, n).wait_send()


def gradients(acts, aTs, dgs, dus, dhs):
    layers = len(acts)
    ff, tokens = acts[0].shape
    d = aTs[0].shape[0]
    vmem = pl.BlockSpec(memory_space=pltpu.VMEM)
    hbm = pl.BlockSpec(memory_space=pl.ANY)
    dma = pltpu.SemaphoreType.DMA
    w, t = 2 * layers, layers
    units = 3 * layers
    wr, tr = d // N, ff // N
    return pl.pallas_call(
        functools.partial(gradient_kernel, layers),
        out_shape=[pltpu.VMEM(s, BF16) for s in ((layers, wr, ff), (layers, wr, ff), (layers, tr, d))],
        in_specs=[hbm] * (5 * layers),
        out_specs=[vmem] * 3,
        scratch_shapes=[
            pltpu.VMEM((w, d, ff), BF16),
            pltpu.VMEM((t, ff, d), BF16),
            pltpu.VMEM((w, 2, Z, wr, ff), BF16),
            pltpu.VMEM((w, Z, wr, ff), BF16),
            pltpu.VMEM((t, Z, tr, d), BF16),
            pltpu.VMEM((w, Z + 1, wr, ff), BF16),
            pltpu.VMEM((t, Z + 1, tr, d), BF16),
            pltpu.VMEM((t, 2, Z, tr, d), BF16),
            pltpu.VMEM((2, ff // (2 * Z), tokens), BF16),
            pltpu.VMEM((2, tokens, TILE), BF16),
            pltpu.VMEM((d, tokens), BF16),
            pltpu.VMEM((tokens, d), BF16),
            pltpu.VMEM((wr, ff), F32),
            pltpu.VMEM((tr, d), F32),
            dma((2,)),
            dma((2,)),
            dma((units, 2, Z)),
            dma((units, 2, Z)),
            dma((units, Z)),
            dma((units, Z)),
            dma((units, Z)),
            dma((units, Z + 1)),
        ],
        compiler_params=pltpu.CompilerParams(collective_id=2, has_side_effects=True, vmem_limit_bytes=60 * 1024 * 1024),
        name="gradients",
    )(*acts, *aTs, *dgs, *dus, *dhs)


def dot(a, b):
    return jnp.dot(a, b, preferred_element_type=F32)


def dot_t(a, b):
    return lax.dot_general(a, b, (((1,), (1,)), ((), ())), preferred_element_type=F32)


CHUNK = 256


def tokens_kernel(layers, x_ref, dy_ref, *refs):
    given, refs = refs[0:3], refs[3:]
    actT, aT, dg, du = (refs[i * layers : (i + 1) * layers] for i in range(4))
    refs = refs[4 * layers :]
    dh, refs = refs[: layers - 1], refs[layers - 1 :]
    wg, wu, wd, act, silu, slope, sem = refs
    ff = wg.shape[2]
    first = pl.program_id(0) == 0
    held = (wg, wu, wd)

    def load(i, l):
        return pltpu.make_async_copy(given[i].at[l], held[i].at[l], sem.at[i, l])

    @pl.when(first)
    def _():
        for l in range(layers):
            for i in range(3):
                load(i, l).start()

    def ready(l):
        @pl.when(first)
        def _():
            for i in range(3):
                load(i, l).wait()

    saved = []
    h = x_ref[...]
    for l in range(layers):
        wide = h.astype(F32)
        scale = lax.rsqrt(jnp.mean(wide * wide, -1, keepdims=True) + 1e-6)
        a = (wide * scale).astype(BF16)
        saved.append((wide, scale))
        ready(l)
        aT[l][...] = a.T
        for f in range(0, ff, CHUNK):
            at = slice(f, f + CHUNK)
            gate, up = dot(a, wg[l, :, at]), dot(a, wu[l, :, at])
            s = jax.nn.sigmoid(gate)
            mine = gate * s
            now = (mine * up).astype(BF16)
            act[:, at] = now
            actT[l][at, :] = now.T
            silu[l, :, at] = mine
            slope[l, :, at] = up * (s + mine * (1.0 - s))
        if l + 1 < layers:
            h = (h.astype(F32) + dot(act[...], wd[l]).astype(BF16).astype(F32)).astype(BF16)
    d = dy_ref[...]
    for l in reversed(range(layers)):
        wide, scale = saved[l]
        if l + 1 < layers:
            dh[l][...] = d
        for f in range(0, ff, CHUNK):
            at = slice(f, f + CHUNK)
            by_act = dot_t(d, wd[l, at, :]).astype(BF16).astype(F32)
            dg[l][:, at] = (by_act * slope[l, :, at]).astype(BF16)
            du[l][:, at] = (by_act * silu[l, :, at]).astype(BF16)
        if l > 0:
            by_a = dot_t(dg[l][...], wg[l]).astype(BF16).astype(F32) + dot_t(du[l][...], wu[l]).astype(BF16).astype(F32)
            by_a = by_a.astype(BF16).astype(F32)
            pull = jnp.mean(by_a * wide, -1, keepdims=True)
            back = (by_a * scale - wide * (scale * scale * scale * pull)).astype(BF16)
            d = (d.astype(F32) + back.astype(F32)).astype(BF16)


def through(x, dy, wg, wu, wd):
    layers, dm, ff = wg.shape
    tokens = x.shape[0]
    t = 256
    tall, flat = pl.BlockSpec((t, dm), lambda i: (i, 0)), pl.BlockSpec((t, ff), lambda i: (i, 0))
    hbm = pl.BlockSpec(memory_space=pl.ANY)
    shape = lambda *s: jax.ShapeDtypeStruct(s, BF16)
    outs = pl.pallas_call(
        functools.partial(tokens_kernel, layers),
        grid=(tokens // t,),
        in_specs=[tall, tall, hbm, hbm, hbm],
        out_specs=[pl.BlockSpec((ff, t), lambda i: (0, i))] * layers
        + [pl.BlockSpec((dm, t), lambda i: (0, i))] * layers
        + [flat] * (2 * layers)
        + [tall] * (layers - 1),
        out_shape=[shape(ff, tokens)] * layers + [shape(dm, tokens)] * layers + [shape(tokens, ff)] * (2 * layers) + [shape(tokens, dm)] * (layers - 1),
        scratch_shapes=[pltpu.VMEM(a.shape, BF16) for a in (wg, wu, wd)]
        + [pltpu.VMEM((t, ff), BF16), pltpu.VMEM((layers, t, ff), F32), pltpu.VMEM((layers, t, ff), F32), pltpu.SemaphoreType.DMA((3, layers))],
        compiler_params=pltpu.CompilerParams(dimension_semantics=("arbitrary",), vmem_limit_bytes=63 * 1024 * 1024),
        name="tokens",
    )(x, dy, wg, wu, wd)
    return [list(outs[i * layers : (i + 1) * layers]) for i in range(4)] + [[*outs[4 * layers :], dy]]


def solution(mesh):
    def step(x, dy, *arrays):
        w, m, v = (arrays[i : i + 3] for i in (0, 3, 6))
        g = gradients(*through(x[0], dy[0], *w))
        return tuple(update(g, m, v, w))

    opt = P(None, "dp", None)
    return jax.shard_map(
        step,
        mesh=mesh,
        in_specs=(P(("rep", "dp")), P(("rep", "dp")), P(), P(), P(), *[opt] * 6),
        out_specs=(*[P("rep")] * 3, *[P("rep", "dp")] * 6),
        check_vma=False,
    )
```

```python
import functools

import jax
import jax.numpy as jnp
from jax import lax
from jax.experimental import pallas as pl
from jax.experimental.pallas import tpu as pltpu
from jax.sharding import PartitionSpec as P

MESH = pl.DeviceIdType.MESH
Y, Z, C = 2, 4, 2
N = Y * Z * C
F32, BF16 = jnp.float32, jnp.bfloat16


def place():
    me = lax.axis_index("dp")
    return me, me // (Z * C), lax.rem(me // C, Z), lax.rem(me, C)


def index(y, z, c):
    return (y * Z + z) * C + c


def remote(src, dst, send, recv, to):
    return pltpu.make_async_remote_copy(
        src_ref=src, dst_ref=dst, send_sem=send, recv_sem=recv, device_id={"dp": to}, device_id_type=MESH
    )


def update_kernel(count, layers, *refs):
    g, m, v, wf = refs[0:3], refs[3:6], refs[6:9], refs[9:12]
    full, m_out, v_out = refs[12:15], refs[15:18], refs[18:21]
    own, norms = refs[21:24], refs[24]
    in_sem, norm_send, norm_recv, send_z, recv_z, send_y, recv_y, send_c, recv_c = refs[25:]
    me, y, z, c = place()
    rows = [ref.shape[1] for ref in g]
    loads = []
    for i in range(3):
        loads.append(pltpu.make_async_copy(wf[i].at[:, pl.ds(me * rows[i], rows[i])], own[i], in_sem.at[i]))
        loads[-1].start()

    barrier = pltpu.get_barrier_semaphore()

    def hello(d, _):
        pl.semaphore_signal(barrier, inc=1, device_id={"dp": lax.rem(me + d, N)}, device_id_type=MESH)
        return 0

    lax.fori_loop(1, N, hello, 0)

    total = jnp.zeros((), F32)
    for i in range(3):
        columns = g[i].shape[2]

        def squares(t, acc):
            for l in range(layers):
                part = g[i][l, pl.ds(pl.multiple_of(t * 16, 16), 16), :].astype(F32)
                acc = acc + part * part
            return acc

        acc = lax.fori_loop(0, rows[i] // 16, squares, jnp.zeros((16, columns), F32))
        total = total + jnp.sum(acc)
    norms[pl.ds(me, 1)] = jnp.full((1, 8, 128), total, F32)
    pl.semaphore_wait(barrier, N - 1)

    def tell(d):
        to = lax.rem(me + d, N)
        return remote(norms.at[pl.ds(me, 1)], norms.at[pl.ds(me, 1)], norm_send.at[d], norm_recv.at[d], to)

    lax.fori_loop(1, N, lambda d, _: (tell(d).start(), 0)[1], 0)

    def heard(d, _):
        frm = lax.rem(me + N - d, N)
        copy = remote(norms.at[pl.ds(frm, 1)], norms.at[pl.ds(frm, 1)], norm_send.at[d], norm_recv.at[d], frm)
        copy.wait_recv()
        return 0

    lax.fori_loop(1, N, heard, 0)
    sum_of_squares = jnp.sum(norms[...], axis=0)
    factor = jnp.minimum(1.0, 0.5 * lax.rsqrt(sum_of_squares / count + 1e-30))[0:1, 0:1]
    for load in loads:
        load.wait()
    chunks = [(i, l) for l in range(layers) for i in range(3)]
    mixed = {len(chunks) - 1}

    def block(k, yy, zz, cc):
        i, l = chunks[k]
        return full[i].at[l, pl.ds(index(yy, zz, cc) * rows[i], rows[i])]

    def origin(slot):
        return z - slot if slot < 4 else z + slot - 3

    def has(slot):
        if slot == 0:
            return z >= 0
        return z >= slot if slot < 4 else z + slot - 3 < Z

    def to_y(k, slot):
        ref = block(k, y, origin(slot), c)
        return remote(ref, ref, send_y.at[k, slot], recv_y.at[k, slot], index(1 - y, z, c))

    def from_y(k, slot):
        ref = block(k, 1 - y, origin(slot), c)
        return remote(ref, ref, send_y.at[k, slot], recv_y.at[k, slot], index(1 - y, z, c))

    def to_c(k, side, slot):
        ref = block(k, y if side == 0 else 1 - y, origin(slot), c)
        return remote(ref, ref, send_c.at[k, side, slot], recv_c.at[k, side, slot], index(y, z, 1 - c))

    def from_c(k, side, slot):
        ref = block(k, y if side == 0 else 1 - y, origin(slot), 1 - c)
        return remote(ref, ref, send_c.at[k, side, slot], recv_c.at[k, side, slot], index(y, z, 1 - c))

    lanes = [(k, 0) for k in range(len(chunks))] + [(k, 1) for k in sorted(mixed)]

    def line(n, slot, up):
        k, side = lanes[n]
        ref = block(k, y if side == 0 else 1 - y, origin(slot), c)
        hop = (slot if slot else 0) if up else (slot - 3 if slot else 0)
        return remote(ref, ref, send_z.at[n, 0 if up else 1, hop], recv_z.at[n, 0 if up else 1, hop],
                      index(y, jnp.minimum(z + 1, Z - 1) if up else jnp.maximum(z - 1, 0), c))

    def arrived(n, slot):
        k, side = lanes[n]
        up = slot < 4
        ref = block(k, y if side == 0 else 1 - y, origin(slot), c)
        hop = slot - 1 if up else slot - 4
        return remote(ref, ref, send_z.at[n, 0 if up else 1, hop], recv_z.at[n, 0 if up else 1, hop],
                      index(y, jnp.maximum(z - 1, 0) if up else jnp.minimum(z + 1, Z - 1), c))

    def when(ok, f):
        pl.when(ok)(f)

    waits = []

    def launch(ok, copy):
        when(ok, lambda: copy().start())
        waits.append((ok, copy))

    def spread(n, slot):
        k, side = lanes[n]
        ok = has(slot)
        if slot < 4:
            launch(ok & (z < Z - 1), lambda: line(n, slot, True))
        if slot == 0 or slot >= 4:
            launch(ok & (z > 0), lambda: line(n, slot, False))
        if side == 0 and (k not in mixed or slot == 0):
            launch(ok, lambda: to_y(k, slot))
        launch(ok, lambda: to_c(k, side, slot))

    order = sorted(range(len(chunks)), key=lambda k: k not in mixed)
    def renew(i, l):
        def adamw(t, _):
            at = pl.ds(pl.multiple_of(t * 16, 16), 16)
            grad = g[i][l, at, :].astype(F32) * factor
            w = own[i][l, at, :].astype(F32)
            mm = 0.9 * m[i][l, at, :] + 0.1 * grad
            vv = 0.95 * v[i][l, at, :] + 0.05 * grad * grad
            m_out[i][l, at, :] = mm
            v_out[i][l, at, :] = vv
            new = (w - 0.02 * (mm * lax.rsqrt(vv + 1e-8) + 0.1 * w)).astype(BF16)
            full[i][l, pl.ds(pl.multiple_of(me * rows[i] + t * 16, 16), 16), :] = new
            return 0

        lax.fori_loop(0, rows[i] // 16, adamw, 0)

    for k in order:
        renew(*chunks[k])
        spread(k, 0)
    for k in sorted(mixed):
        from_y(k, 0).wait_recv()
        spread(lanes.index((k, 1)), 0)
    ranked = sorted(range(len(lanes)), key=lambda n: lanes[n][0] in mixed)
    for hop in range(1, Z):
        for n in ranked:
            for slot in (hop, hop + 3):
                when(has(slot), lambda: arrived(n, slot).wait_recv())
                spread(n, slot)

    slots = [0, 1, 4, 2, 5, 3, 6]
    for k in order:
        for slot in slots:
            when(has(slot), lambda: from_c(k, 0, slot).wait_recv())
    for slot in slots:
        for k in order:
            if k not in mixed:
                when(has(slot), lambda: from_y(k, slot).wait_recv())
                launch(has(slot), lambda k=k, slot=slot: to_c(k, 1, slot))
    for k in order:
        for slot in slots:
            when(has(slot), lambda: from_c(k, 1, slot).wait_recv())
    for ok, copy in waits:
        when(ok, lambda: copy().wait_send())
    lax.fori_loop(1, N, lambda d, _: (tell(d).wait_send(), 0)[1], 0)


def update(g, m, v, w):
    layers = w[0].shape[0]
    count = float(sum(a.size for a in w))
    vmem = pl.BlockSpec(memory_space=pltpu.VMEM)
    hbm = pl.BlockSpec(memory_space=pl.ANY)
    chunks = 3 * layers
    dma = pltpu.SemaphoreType.DMA
    outs = [pltpu.VMEM(a.shape, BF16) for a in w] + [jax.ShapeDtypeStruct(a.shape, F32) for a in (*m, *v)]
    return pl.pallas_call(
        functools.partial(update_kernel, count, layers),
        out_shape=outs,
        in_specs=[vmem] * 9 + [hbm] * 3,
        out_specs=[vmem] * 9,
        scratch_shapes=[pltpu.VMEM(a.shape, BF16) for a in g]
        + [pltpu.VMEM((N, 8, 128), F32)]
        + [dma((3,)), dma((N,)), dma((N,)), dma((chunks + 1, 2, Z)), dma((chunks + 1, 2, Z)), dma((chunks, 7)), dma((chunks, 7)),
           dma((chunks, 2, 7)), dma((chunks, 2, 7))],
        compiler_params=pltpu.CompilerParams(collective_id=1, has_side_effects=True, vmem_limit_bytes=36 * 1024 * 1024),
        name="update",
    )(*g, *m, *v, *w)


TILE = 256


def gradient_kernel(layers, *refs):
    acts, aTs, dgs, dus, dhs = (refs[i * layers : (i + 1) * layers] for i in range(5))
    refs = refs[5 * layers :]
    outs, refs = refs[0:3], refs[3:]
    wide, tall, from_c, wide_y, tall_y, wide_z, tall_z, tall_c = refs[:8]
    left, right, aT, dh, wide_sum, tall_sum = refs[8:14]
    tile_sem, keep_sem, send_c, recv_c, send_y, recv_y, send_z, recv_z = refs[14:]
    me, y, z, c = place()
    partner, across = index(y, z, 1 - c), index(1 - y, z, c)
    above, below = index(y, jnp.minimum(z + 1, Z - 1), c), index(y, jnp.maximum(z - 1, 0), c)

    units = []
    for l in reversed(range(layers)):
        units += [(2, l, l), (0, l, 2 * l), (1, l, 2 * l + 1)]
    tiles = [2 * Z if i == 2 else dgs[l].shape[1] // TILE for i, l, _ in units]
    tall_tile = acts[0].shape[0] // (2 * Z)

    def rows_of(t):
        return pl.ds(pl.multiple_of(lax.rem(t + Z * (1 - y), 2 * Z) * tall_tile, tall_tile), tall_tile)

    def tile(k, t, slot):
        i, l, _ = units[k]
        if i == 2:
            return pltpu.make_async_copy(acts[l].at[rows_of(t), :], left.at[slot], tile_sem.at[slot])
        at = pl.ds(pl.multiple_of(t * TILE, TILE), TILE)
        return pltpu.make_async_copy((dgs, dus)[i][l].at[:, at], right.at[slot], tile_sem.at[slot])

    def keep(k):
        i, l, _ = units[k]
        if i == 2:
            return pltpu.make_async_copy(dhs[l], dh, keep_sem.at[0])
        return pltpu.make_async_copy(aTs[l], aT, keep_sem.at[1])

    def unit(k, start, stop):
        i, l, s = units[k]

        def body(t, _):
            slot = lax.rem(t, 2)

            @pl.when(t + 1 < tiles[k])
            def _():
                tile(k, t + 1, 1 - slot).start()

            tile(k, t, slot).wait()
            at = pl.ds(pl.multiple_of(t * TILE, TILE), TILE)
            if i == 2:
                tall[s, rows_of(t), :] = jnp.dot(left[slot], dh[...], preferred_element_type=F32).astype(BF16)
            else:
                wide[s, :, at] = jnp.dot(aT[...], right[slot], preferred_element_type=F32).astype(BF16)
            return 0

        lax.fori_loop(start, stop, body, 0)

    def parts(k):
        i, l, s = units[k]
        if i == 2:
            return tall.at[s], tall_c.at[s], tall_y.at[s], tall_z.at[s], tall_sum
        return wide.at[s], from_c.at[s], wide_y.at[s], wide_z.at[s], wide_sum

    def block(k, yy, zz, cc):
        ref = parts(k)[0]
        rows = ref.shape[0] // N
        return ref.at[pl.ds(pl.multiple_of(index(yy, zz, cc) * rows, rows), rows), :]

    def by_rows(rows, f):
        def body(t, _):
            f(pl.ds(pl.multiple_of(t * 16, 16), 16))
            return 0

        lax.fori_loop(0, rows // 16, body, 0)

    end = (z == 0) | (z == Z - 1)

    def piece(n):
        far = (jnp.where(z < 2, Z - 1, 0), jnp.where(end, jnp.where(z == 0, 2, 1), jnp.where(z == 1, 0, Z - 1)), jnp.where(end, Z - 2 - jnp.where(z == 0, 1, 0), 3 - z), z)
        return far[n]

    def swap(k, half, n):
        zz = piece(n)
        row = 1 - y if half == 0 else y
        return remote(block(k, row, zz, 1 - c), parts(k)[1].at[half, zz], send_c.at[k, half, n], recv_c.at[k, half, n], partner)

    def cross(k, n):
        zz = piece(n)
        return remote(block(k, 1 - y, zz, c), parts(k)[2].at[zz], send_y.at[k, n], recv_y.at[k, n], across)

    def pass_on(k, n):
        zz = piece(n)
        slot = jnp.where(z - 1 == zz, Z, zz)
        return remote(block(k, y, zz, c), parts(k)[3].at[slot], send_z.at[k, n], recv_z.at[k, slot], jnp.where(zz > z, above, below))

    def passed(k, slot):
        ref = parts(k)[3].at[slot]
        return remote(ref, ref, send_z.at[k, 0], recv_z.at[k, slot], jnp.where(end, jnp.where(z == 0, above, below), above))

    def step1(k, half):
        for n in range(Z):
            swap(k, half, n).start()

    def step2(k):
        got = parts(k)[1]
        for n in range(Z):
            zz = piece(n)
            swap(k, 0, n).wait_recv()
            mine = block(k, 1 - y, zz, c)

            def add(at):
                mine[at, :] = (mine[at, :].astype(F32) + got[0, zz, at, :].astype(F32)).astype(BF16)

            by_rows(mine.shape[0], add)
            cross(k, n).start()

    def gather(k, n):
        _, got, over, _, total = parts(k)
        zz = piece(n)
        swap(k, 1, n).wait_recv()
        cross(k, n).wait_recv()
        mine = block(k, y, zz, c)

        def first(at):
            total[at, :] = mine[at, :].astype(F32) + got[1, zz, at, :].astype(F32) + over[zz, at, :].astype(F32)

        by_rows(mine.shape[0], first)
        return mine, total

    def also(k, ok, slot):
        _, _, _, came, total = parts(k)

        @pl.when(ok)
        def _():
            passed(k, slot).wait_recv()

            def add(at):
                total[at, :] += came[slot, at, :].astype(F32)

            by_rows(total.shape[0], add)

    def step3(k, ends, places=(0, 1, 2)):
        @pl.when(end if ends else jnp.logical_not(end))
        def _():
            for n in places:
                mine, total = gather(k, n)
                if not ends:
                    also(k, z >= 0, piece(n))

                def store(at):
                    mine[at, :] = total[at, :].astype(BF16)

                by_rows(mine.shape[0], store)
                pass_on(k, n).start()

    def step4(k):
        i, l, _ = units[k]
        mine, total = gather(k, Z - 1)
        also(k, z > 0, z)
        also(k, z < Z - 1, Z)

        def store(at):
            outs[i][l, at, :] = total[at, :].astype(BF16)

        by_rows(mine.shape[0], store)

    tile(0, 0, 0).start()
    keep(0).start()
    keep(1).start()
    barrier = pltpu.get_barrier_semaphore()
    near = [(partner, z >= 0), (across, z >= 0), (above, z < Z - 1), (below, z > 0)]
    for to, ok in near:

        @pl.when(ok)
        def _():
            pl.semaphore_signal(barrier, inc=1, device_id={"dp": to}, device_id_type=MESH)

    for k in range(len(units)):
        if k > 0:
            tile(k, 0, 0).start()
        if units[k][0] == 2 or units[k][0] == 0:
            if k > 1:
                keep(k).start()
            keep(k).wait()
        if k == 0:
            unit(k, 0, Z)
            pl.semaphore_wait(barrier, 2 + (z < Z - 1).astype(jnp.int32) + (z > 0).astype(jnp.int32))
            step1(k, 0)
            unit(k, Z, Z + 2)
            step2(k)
            unit(k, Z + 2, tiles[k])
            step1(k, 1)
        elif k == 1:
            unit(k, 0, tiles[k])
            step1(k, 0)
            step1(k, 1)
        else:
            unit(k, 0, 3)
            step2(k - 1)
            if k > 3:
                step3(k - 4, False, (0,))
            unit(k, 3, tiles[k])
            step1(k, 0)
            step1(k, 1)
            if k > 3:
                step3(k - 4, False, (1, 2))
            if k > 2:
                step3(k - 3, True)
    last = len(units) - 1
    step2(last)
    step3(last - 3, False)
    for k in range(last - 2, len(units)):
        step3(k, True)
        step3(k, False)
        step4(k - 3)
    for k in range(last - 2, len(units)):
        step4(k)
    for k in range(len(units)):
        for n in range(Z):
            swap(k, 0, n).wait_send()
            swap(k, 1, n).wait_send()
            cross(k, n).wait_send()
            if n < Z - 1:
                pass_on(k, n).wait_send()


def gradients(acts, aTs, dgs, dus, dhs):
    layers = len(acts)
    ff, tokens = acts[0].shape
    d = aTs[0].shape[0]
    vmem = pl.BlockSpec(memory_space=pltpu.VMEM)
    hbm = pl.BlockSpec(memory_space=pl.ANY)
    dma = pltpu.SemaphoreType.DMA
    w, t = 2 * layers, layers
    units = 3 * layers
    wr, tr = d // N, ff // N
    return pl.pallas_call(
        functools.partial(gradient_kernel, layers),
        out_shape=[pltpu.VMEM(s, BF16) for s in ((layers, wr, ff), (layers, wr, ff), (layers, tr, d))],
        in_specs=[hbm] * (5 * layers),
        out_specs=[vmem] * 3,
        scratch_shapes=[
            pltpu.VMEM((w, d, ff), BF16),
            pltpu.VMEM((t, ff, d), BF16),
            pltpu.VMEM((w, 2, Z, wr, ff), BF16),
            pltpu.VMEM((w, Z, wr, ff), BF16),
            pltpu.VMEM((t, Z, tr, d), BF16),
            pltpu.VMEM((w, Z + 1, wr, ff), BF16),
            pltpu.VMEM((t, Z + 1, tr, d), BF16),
            pltpu.VMEM((t, 2, Z, tr, d), BF16),
            pltpu.VMEM((2, ff // (2 * Z), tokens), BF16),
            pltpu.VMEM((2, tokens, TILE), BF16),
            pltpu.VMEM((d, tokens), BF16),
            pltpu.VMEM((tokens, d), BF16),
            pltpu.VMEM((wr, ff), F32),
            pltpu.VMEM((tr, d), F32),
            dma((2,)),
            dma((2,)),
            dma((units, 2, Z)),
            dma((units, 2, Z)),
            dma((units, Z)),
            dma((units, Z)),
            dma((units, Z)),
            dma((units, Z + 1)),
        ],
        compiler_params=pltpu.CompilerParams(collective_id=2, has_side_effects=True, vmem_limit_bytes=60 * 1024 * 1024),
        name="gradients",
    )(*acts, *aTs, *dgs, *dus, *dhs)


def dot(a, b):
    return jnp.dot(a, b, preferred_element_type=F32)


def dot_t(a, b):
    return lax.dot_general(a, b, (((1,), (1,)), ((), ())), preferred_element_type=F32)


CHUNK = 256


def tokens_kernel(layers, x_ref, dy_ref, *refs):
    given, refs = refs[0:3], refs[3:]
    actT, aT, dg, du = (refs[i * layers : (i + 1) * layers] for i in range(4))
    refs = refs[4 * layers :]
    dh, refs = refs[: layers - 1], refs[layers - 1 :]
    wg, wu, wd, act, silu, slope, sem = refs
    ff = wg.shape[2]
    first = pl.program_id(0) == 0
    held = (wg, wu, wd)

    def load(i, l):
        return pltpu.make_async_copy(given[i].at[l], held[i].at[l], sem.at[i, l])

    @pl.when(first)
    def _():
        for l in range(layers):
            for i in range(3):
                load(i, l).start()

    def ready(l):
        @pl.when(first)
        def _():
            for i in range(3):
                load(i, l).wait()

    saved = []
    h = x_ref[...]
    for l in range(layers):
        wide = h.astype(F32)
        scale = lax.rsqrt(jnp.mean(wide * wide, -1, keepdims=True) + 1e-6)
        a = (wide * scale).astype(BF16)
        saved.append((wide, scale))
        ready(l)
        aT[l][...] = a.T
        for f in range(0, ff, CHUNK):
            at = slice(f, f + CHUNK)
            gate, up = dot(a, wg[l, :, at]), dot(a, wu[l, :, at])
            s = jax.nn.sigmoid(gate)
            mine = gate * s
            now = (mine * up).astype(BF16)
            act[:, at] = now
            actT[l][at, :] = now.T
            silu[l, :, at] = mine
            slope[l, :, at] = up * (s + mine * (1.0 - s))
        if l + 1 < layers:
            h = (h.astype(F32) + dot(act[...], wd[l]).astype(BF16).astype(F32)).astype(BF16)
    d = dy_ref[...]
    for l in reversed(range(layers)):
        wide, scale = saved[l]
        if l + 1 < layers:
            dh[l][...] = d
        for f in range(0, ff, CHUNK):
            at = slice(f, f + CHUNK)
            by_act = dot_t(d, wd[l, at, :]).astype(BF16).astype(F32)
            dg[l][:, at] = (by_act * slope[l, :, at]).astype(BF16)
            du[l][:, at] = (by_act * silu[l, :, at]).astype(BF16)
        if l > 0:
            by_a = dot_t(dg[l][...], wg[l]).astype(BF16).astype(F32) + dot_t(du[l][...], wu[l]).astype(BF16).astype(F32)
            by_a = by_a.astype(BF16).astype(F32)
            pull = jnp.mean(by_a * wide, -1, keepdims=True)
            back = (by_a * scale - wide * (scale * scale * scale * pull)).astype(BF16)
            d = (d.astype(F32) + back.astype(F32)).astype(BF16)


def through(x, dy, wg, wu, wd):
    layers, dm, ff = wg.shape
    tokens = x.shape[0]
    t = 256
    tall, flat = pl.BlockSpec((t, dm), lambda i: (i, 0)), pl.BlockSpec((t, ff), lambda i: (i, 0))
    hbm = pl.BlockSpec(memory_space=pl.ANY)
    shape = lambda *s: jax.ShapeDtypeStruct(s, BF16)
    outs = pl.pallas_call(
        functools.partial(tokens_kernel, layers),
        grid=(tokens // t,),
        in_specs=[tall, tall, hbm, hbm, hbm],
        out_specs=[pl.BlockSpec((ff, t), lambda i: (0, i))] * layers
        + [pl.BlockSpec((dm, t), lambda i: (0, i))] * layers
        + [flat] * (2 * layers)
        + [tall] * (layers - 1),
        out_shape=[shape(ff, tokens)] * layers + [shape(dm, tokens)] * layers + [shape(tokens, ff)] * (2 * layers) + [shape(tokens, dm)] * (layers - 1),
        scratch_shapes=[pltpu.VMEM(a.shape, BF16) for a in (wg, wu, wd)]
        + [pltpu.VMEM((t, ff), BF16), pltpu.VMEM((layers, t, ff), F32), pltpu.VMEM((layers, t, ff), F32), pltpu.SemaphoreType.DMA((3, layers))],
        compiler_params=pltpu.CompilerParams(dimension_semantics=("arbitrary",), vmem_limit_bytes=63 * 1024 * 1024),
        name="tokens",
    )(x, dy, wg, wu, wd)
    return [list(outs[i * layers : (i + 1) * layers]) for i in range(4)] + [[*outs[4 * layers :], dy]]


def solution(mesh):
    def step(x, dy, *arrays):
        w, m, v = (arrays[i : i + 3] for i in (0, 3, 6))
        g = gradients(*through(x[0], dy[0], *w))
        return tuple(update(g, m, v, w))

    opt = P(None, "dp", None)
    return jax.shard_map(
        step,
        mesh=mesh,
        in_specs=(P(("rep", "dp")), P(("rep", "dp")), P(), P(), P(), *[opt] * 6),
        out_specs=(*[P("rep")] * 3, *[P("rep", "dp")] * 6),
        check_vma=False,
    )
```
